256 devices in a mesh: hi: 8 (over y, core), lo: 32 (over z, x).
Axes of the slice: x: 4, y: 4, z: 8, core: 2. Of those that a mesh axis runs over, the one named last changes fastest.
Arguments:
- grm: bfloat16 [8, 32, 64, 8, 2048], P(None, 'lo', None, 'hi'), as said below
- right_sides: float32 [16384, 512], P(('hi', 'lo')), may hold values from -6 to 6
- inv_diag: float32 [16384], P(('hi', 'lo')), may hold values from 0.3 to 1
- bases: float32 [16384, 576], P(('hi', 'lo')), may hold values from -0.75 to 0.75
- couplings: float32 [9, 64, 64], replicated, as said below
- level_map: int32 [8], replicated, may hold values from 0 to 7, each once
- variance: float32 [2], replicated, may hold values from 0.3 to 1.5
- iters_per_column: int32 [512], replicated, may hold values from 1 to 3
Outputs:
- solution: float32 [16384, 512], P(('hi', 'lo'))
- residual: float32 [16384, 512], P(('hi', 'lo'))
The draws below stay inside these ranges and needn't reach their ends.
Inputs may be any that keep to these rules, and one draw needn't show every extreme that they name: `grm`: G is symmetric and positive definite. `couplings`: each of the 9 matrices is symmetric and positive definite. `level_map`: a permutation of the levels.
All inputs are finite; a program needn't handle non-finite values.
Results may differ from the reference program's by a relative error of at most 0.0055.
Values may be sent and summed in bfloat16 or wider, within the bound.
No kernel may reach another device: no remote copies, remote signals or barrier semaphores. Data moves between devices by JAX's collectives and lax.ppermute only.
A program may use at most 64 MiB of HBM per device.

```python
import math
import jax
import jax.numpy as jnp
from jax import lax

ROWS_DEV = 64
RHS = 512
RANK = 64
LEVELS = 8
ITERS = 3
HI_BLOCKS = 8
LO_BLOCKS = 32
SAMPLES = 16384
N_HI = 8
N_LO = 32


def draw_grm(key, part):
    entries = jax.random.normal(key, (SAMPLES, SAMPLES), jnp.float32)
    spread = 0.45 / math.sqrt(2.0 * SAMPLES)
    symmetric = (entries + entries.T) * spread + jnp.eye(SAMPLES, dtype=jnp.float32)
    return symmetric.astype(jnp.bfloat16).reshape(HI_BLOCKS, LO_BLOCKS, ROWS_DEV, HI_BLOCKS, LO_BLOCKS * ROWS_DEV)


def draw_couplings(key, part):
    factors = jax.random.normal(jax.random.fold_in(key, 11), (LEVELS + 1, RANK, RANK), jnp.float32)
    low_end = math.log(0.3)
    high_end = math.log(1.0)
    level_scale = jnp.exp(jax.random.uniform(jax.random.fold_in(key, 12), (LEVELS + 1,), jnp.float32, low_end, high_end))
    gram = jnp.einsum('lij,lkj->lik', factors, factors, precision=lax.Precision.HIGHEST) / RANK
    gram = gram + 0.25 * jnp.eye(RANK, dtype=jnp.float32)[None]
    return gram * level_scale[:, None, None]


def place_ends(result, rng, least, high):
    index_at = [jax.random.randint(jax.random.fold_in(rng, axis), (), 0, length) for axis, length in enumerate(result.shape)]
    widest = result.shape.index(max(result.shape))
    beside = index_at[:widest] + [(index_at[widest] + 1) % result.shape[widest]] + index_at[widest + 1:]
    return result.at[tuple(index_at)].set(least).at[tuple(beside)].set(high)


def block_scale(key, dims, cuts, smallest, top_value):
    level, own = 1.0, jax.random.fold_in(key, 6)
    for position, shards_of in cuts:
        steps = jnp.exp(jax.random.uniform(jax.random.fold_in(own, position), (shards_of,), jnp.float32, smallest / len(cuts), top_value / len(cuts)))
        level = level * jnp.repeat(steps, dims[position] // shards_of).reshape([-1 if axis == position else 1 for axis in range(len(dims))])
    return level


def noise(stream_key, dims, scale, most, cuts=(), held_as=jnp.bfloat16):
    gain = block_scale(stream_key, dims, cuts, -0.22, 0.18) if cuts else 1.0
    values = jax.random.normal(stream_key, dims, jnp.float32) * scale * gain
    return jnp.minimum(jnp.maximum(values, -most), most).astype(held_as)


def setup_inputs(seed: int = 0) -> dict:
    key_of = jax.random.split(jax.random.key(seed), 9)
    return {
        "grm": draw_grm(jax.random.fold_in(key_of[8], 71), 0),
        "right_sides": noise(key_of[1], (SAMPLES, RHS), 1.0, 6.0, ((0, 256),), jnp.float32),
        "inv_diag": jnp.clip(jnp.exp(math.log(1.0) - 1.2039728 * jax.random.uniform(key_of[2], (SAMPLES,), jnp.float32) ** block_scale(key_of[2], (SAMPLES,), ((0, 256),), -0.2, 0.2)), 0.3, 1.0),
        "bases": noise(key_of[3], (SAMPLES, (LEVELS + 1) * RANK), ROWS_DEV ** -0.5, 0.75, ((0, 256),), jnp.float32),
        "couplings": draw_couplings(jax.random.fold_in(key_of[8], 71), 0),
        "level_map": jax.random.permutation(key_of[5], LEVELS).astype(jnp.int32),
        "variance": jnp.clip(jnp.exp(jax.random.uniform(key_of[6], (2,), jnp.float32, math.log(0.3), math.log(1.5))), 0.3, 1.5),
        "iters_per_column": place_ends(jax.random.randint(key_of[7], (RHS,), 1, ITERS + 1), jax.random.fold_in(key_of[7], 1), 1, ITERS).astype(jnp.int32),
    }


def apply_system(grm, direction, variance):
    matrix = grm.reshape(SAMPLES, SAMPLES)
    product = jnp.dot(matrix, direction.astype(jnp.bfloat16), preferred_element_type=jnp.float32)
    return variance[0] * product + variance[1] * direction


def precondition(resid, inv_diag, bases, couplings, level_map):
    blocks = N_HI * N_LO
    bit_count = blocks.bit_length() - 1
    level_total = LEVELS + 1
    resid_blocks = resid.reshape(blocks, ROWS_DEV, RHS)
    basis_blocks = bases.reshape(blocks, ROWS_DEV, level_total * RANK)
    coefficients = jnp.einsum("dnk,dnb->dkb", basis_blocks, resid_blocks, precision=lax.Precision.HIGHEST)
    coefficients = coefficients.reshape(blocks, level_total, RANK, RHS)
    stacked = jnp.zeros_like(coefficients)
    order = jnp.arange(blocks, dtype=jnp.int32)
    level_ids = jnp.arange(level_total, dtype=jnp.int32)
    for bit_index in range(bit_count):
        level = level_map[bit_index]
        partner = jnp.bitwise_xor(order, 1 << bit_index).astype(jnp.int32)
        chosen = jnp.take(coefficients, level, axis=1)
        summed = chosen + jnp.take(chosen, partner, axis=0)
        matrix = jnp.take(couplings, level, axis=0)
        term = jnp.einsum("rs,dsb->drb", matrix, summed, precision=lax.Precision.HIGHEST)
        select = (level_ids == level).astype(jnp.float32)
        stacked = stacked + select[None, :, None, None] * term[:, None]
    total = jnp.sum(coefficients[:, LEVELS], axis=0)
    coarse = jnp.dot(couplings[LEVELS], total, precision=lax.Precision.HIGHEST)
    stacked = stacked.at[:, LEVELS].add(coarse[None])
    lifted = jnp.einsum("dnk,dkb->dnb", basis_blocks, stacked.reshape(blocks, level_total * RANK, RHS), precision=lax.Precision.HIGHEST)
    return inv_diag[:, None] * resid + lifted.reshape(SAMPLES, RHS)


def reference(grm, right_sides, inv_diag, bases, couplings, level_map, variance, iters_per_column):
    solution = jnp.zeros_like(right_sides)
    residual = right_sides
    scaled = precondition(residual, inv_diag, bases, couplings, level_map)
    direction = scaled
    energy = jnp.sum(residual * scaled, axis=0)
    for step in range(ITERS):
        image = apply_system(grm, direction, variance)
        curvature = jnp.sum(direction * image, axis=0)
        alpha = energy / curvature
        stepsize = jnp.where(step < iters_per_column, alpha, jnp.zeros_like(alpha))
        solution = solution + stepsize * direction
        residual = residual - stepsize * image
        if step + 1 < ITERS:
            scaled = precondition(residual, inv_diag, bases, couplings, level_map)
            fresh = jnp.sum(residual * scaled, axis=0)
            direction = scaled + (fresh / energy) * direction
            energy = fresh
    return solution, residual
```

```python
import jax
import jax.numpy as jnp
from jax import lax
from jax.sharding import Mesh
from jax.sharding import PartitionSpec as P


HI = ("y", "c")
LO = ("z", "x")
HI_LO = ("y", "c", "z", "x")
BF16 = jnp.bfloat16
F32 = jnp.float32
EXACT = lax.Precision.HIGHEST


def mm(left, right):
    return jnp.dot(left, right, precision=EXACT)


def tmm(left, right):
    return lax.dot_general(left, right, (((0,), (0,)), ((), ())), precision=EXACT)


def copies_of_all(array, axes):
    copies = jnp.broadcast_to(array, (lax.axis_size(axes), *array.shape))
    return lax.all_to_all(copies, axes, split_axis=0, concat_axis=0, tiled=True)


def from_partner(value, axes, bit):
    pairs = [(source, source ^ (1 << bit)) for source in range(lax.axis_size(axes))]
    return lax.ppermute(value, axes, pairs)


def local(grm, right_sides, inv_diag, bases, couplings, level_map, variance, iters_per_column):
    rows, rhs = right_sides.shape
    levels = couplings.shape[0] - 1
    rank = couplings.shape[1]
    n_hi, n_lo = lax.axis_size(HI), lax.axis_size(LO)
    lo_bits = n_lo.bit_length() - 1
    hi_bits = n_hi.bit_length() - 1
    width = rhs + rank
    g_block = grm.reshape(-1, grm.shape[4])
    genetic, noise = variance[0], variance[1]
    me_hi, me_lo = lax.axis_index(HI), lax.axis_index(LO)

    scale = 1.0 / (n_hi * n_lo * jnp.max(jnp.abs(couplings)))
    couplings = couplings * scale
    diag = (inv_diag * scale)[:, None]

    old = jnp.arange(levels * rank, dtype=jnp.int32)
    wanted = jnp.repeat(level_map, rank) * rank + old % rank
    shuffle = (old[:, None] == wanted[None, :]).astype(F32)
    by_bit = mm(bases[:, : levels * rank], shuffle)
    select = (level_map[:, None] == jnp.arange(levels, dtype=jnp.int32)[None, :]).astype(F32)
    coupled = mm(select, couplings[:levels].reshape(levels, rank * rank)).reshape(levels, rank, rank)
    lift = jnp.concatenate(
        [mm(by_bit[:, g * rank : (g + 1) * rank], coupled[g]) for g in range(levels)], axis=1
    )
    coarse_basis = bases[:, levels * rank :]
    coarse_coupling = couplings[levels]

    def precondition(field):
        coefficients = tmm(by_bit, field)
        sent = coefficients.astype(BF16).reshape(levels, rank, -1)
        arrived = [from_partner(sent[g], LO, g) for g in range(lo_bits)]
        arrived += [from_partner(sent[lo_bits + g], HI, g) for g in range(hi_bits)]
        both = coefficients + jnp.concatenate(arrived, axis=0).astype(F32)
        return diag * field + mm(lift, both)

    def gathered(block):
        near = lax.all_gather(block.astype(BF16), "x", axis=0, tiled=True)
        return lax.all_gather(near, "z", axis=0, tiled=True)

    def summed_over_hi(partial):
        partial = partial.reshape(n_hi, -1, partial.shape[-1])
        arrived = lax.all_to_all(partial.astype(BF16), HI, split_axis=0, concat_axis=0, tiled=True)
        own = lax.dynamic_index_in_dim(partial, me_hi, 0, keepdims=False)
        others = jnp.where(
            jnp.arange(n_hi)[:, None, None] == me_hi, jnp.zeros((), F32), arrived.astype(F32)
        )
        return own + others.sum(axis=0)

    def times_g(everyone):
        return jnp.dot(g_block, everyone, preferred_element_type=F32)

    share = rank // n_lo
    parts = tmm(coarse_basis, right_sides).reshape(n_lo, share, rhs)
    own_t = lax.all_to_all(parts, LO, split_axis=0, concat_axis=0, tiled=True).sum(axis=0)

    first = jnp.concatenate([precondition(right_sides), coarse_basis], axis=1)
    all_first = gathered(first)
    first_image = genetic * summed_over_hi(times_g(all_first)) + noise * first

    second = precondition(first_image)
    coarse_image = first_image[:, rhs:]
    all_second = gathered(jnp.concatenate([second, coarse_image], axis=1))
    all_coarse_image = all_second[:, width:]
    second_partial = times_g(all_second[:, :width])

    def coarse_rows(everyone):
        whole = lax.dot_general(
            all_coarse_image, everyone, (((0,), (0,)), ((), ())), preferred_element_type=F32
        )
        return lax.dynamic_slice_in_dim(whole, me_lo * share, share, axis=0)

    def beside(fields, values):
        top = lax.reduce_precision(values, 8, 7)
        rest = values - top
        top = jnp.pad(top, ((0, rows - piece_rows), (0, 0)))
        rest = jnp.pad(rest, ((0, more_rows * (width + rank) // rank - piece_rows), (0, 0)))
        rest = rest.reshape(more_rows, width + rank)
        count = fields.shape[0]
        fields = jnp.concatenate([fields, jnp.broadcast_to(top, (count, rows, rank))], axis=2)
        return jnp.concatenate([fields, jnp.broadcast_to(rest, (count, *rest.shape))], axis=1)

    def taken_apart(sent):
        fields, top = sent[..., :rows, :width], sent[..., :piece_rows, width:]
        rest = sent[..., rows:, :].reshape(*sent.shape[:-2], -1, rank)[..., :piece_rows, :]
        return fields, top.astype(F32) + rest.astype(F32)

    pieces = jnp.concatenate([own_t, coarse_rows(all_first), coarse_rows(all_second[:, :width])], axis=1)
    piece_width = pieces.shape[1]
    pieces = pieces.reshape(-1, rank)
    piece_rows = pieces.shape[0]
    more_rows = -(-piece_rows * rank // ((width + rank) * 8)) * 8
    with_pieces = beside(second_partial.reshape(n_hi, rows, width), pieces)
    second_sum, pieces = taken_apart(summed_over_hi(with_pieces))
    second_image = genetic * second_sum + noise * second

    third = precondition(second_image)
    all_third, table = taken_apart(
        gathered(beside(third[None], pieces)[0]).reshape(n_lo, rows + more_rows, width + rank)
    )
    all_third = all_third.reshape(n_lo * rows, width)
    third_image = genetic * summed_over_hi(times_g(all_third)) + noise * third

    table = table.reshape(rank, piece_width)
    t0 = table[:, :rhs]
    k_first = table[:, rhs : rhs + width]
    k_second = table[:, rhs + width :]
    k_basis = k_first[:, rhs:]
    s0 = mm(coarse_coupling, t0)
    s1 = mm(coarse_coupling, k_first[:, :rhs] + mm(k_basis, s0))
    s2 = mm(coarse_coupling, k_second[:, :rhs] + mm(k_second[:, rhs:], s0) + mm(k_basis, s1))

    v0 = first[:, :rhs] + mm(coarse_basis, s0)
    v1 = second[:, :rhs] + mm(second[:, rhs:], s0) + mm(coarse_basis, s1)
    v2 = third[:, :rhs] + mm(third[:, rhs:], s0) + mm(second[:, rhs:], s1) + mm(coarse_basis, s2)
    w0 = right_sides
    w1 = first_image[:, :rhs] + mm(coarse_image, s0)
    w2 = second_image[:, :rhs] + mm(second_image[:, rhs:], s0) + mm(coarse_image, s1)
    w3 = third_image[:, :rhs] + mm(third_image[:, rhs:], s0)
    w3 = w3 + mm(second_image[:, rhs:], s1) + mm(coarse_image, s2)

    pairs = [(w0, v0), (w1, v0), (w1, v1), (w2, v1), (w2, v2), (w3, v2)]
    moments = jnp.stack([jnp.sum(w * v, axis=0) for w, v in pairs])
    moments = copies_of_all(moments, ("y", "x")).sum(axis=0)
    moments = copies_of_all(moments, ("c", "z")).sum(axis=0)

    m = [moments[k] for k in range(6)]
    one = jnp.ones_like(m[0])
    res, full_res = [one], [one]
    sol, direction, energy = [], [], None
    for step in range(3):
        count = step + 1
        fresh = sum(full_res[p] * full_res[q] * m[p + q] for p in range(count) for q in range(count))
        if step == 0:
            direction = [one]
        else:
            turn = fresh / energy
            direction = [
                full_res[j] + (turn * direction[j] if j < step else 0.0) for j in range(count)
            ]
        energy = fresh
        curvature = sum(
            direction[p] * direction[q] * m[p + q + 1] for p in range(count) for q in range(count)
        )
        alpha = energy / curvature
        active = step < iters_per_column
        before = sol + [jnp.zeros_like(one)]
        sol = [jnp.where(active, before[j] + alpha * direction[j], before[j]) for j in range(count)]
        grown = full_res + [jnp.zeros_like(one)]
        full_res = [grown[0]] + [grown[j + 1] - alpha * direction[j] for j in range(count)]
        kept = res + [jnp.zeros_like(one)]
        res = [jnp.where(active, full_res[j], kept[j]) for j in range(count + 1)]

    solution = sol[0] * v0 + sol[1] * v1 + sol[2] * v2
    residual = w0 + res[1] * w1 + res[2] * w2 + res[3] * w3
    return (solution, residual)


def solution(mesh):
    split = Mesh(mesh.devices.reshape(4, 2, 8, 4), HI_LO)
    return jax.shard_map(
        local,
        mesh=split,
        in_specs=(
            P(None, LO, None, HI, None),
            P(HI_LO, None),
            P(HI_LO),
            P(HI_LO, None),
            P(),
            P(),
            P(),
            P(),
        ),
        out_specs=(P(HI_LO, None), P(HI_LO, None)),
        check_vma=False,
    )
```

```python
import jax
import jax.numpy as jnp
from jax import lax
from jax.sharding import Mesh
from jax.sharding import PartitionSpec as P


HI = ("y", "c")
LO = ("z", "x")
HI_LO = ("y", "c", "z", "x")
COLUMNS = ("c", "z")
ROWS = ("y", "x")
BF16 = jnp.bfloat16
F32 = jnp.float32
EXACT = lax.Precision.HIGHEST
STEPS = 3


def mm(left, right):
    return jnp.dot(left, right, precision=EXACT)


def tmm(left, right):
    return lax.dot_general(left, right, (((0,), (0,)), ((), ())), precision=EXACT)


def from_everyone(array, axes):
    copies = jnp.broadcast_to(array, (lax.axis_size(axes), *array.shape))
    return lax.all_to_all(copies, axes, split_axis=0, concat_axis=0, tiled=True)


def exchanged(array, axes):
    return lax.all_to_all(array, axes, split_axis=0, concat_axis=0, tiled=True)


def shifted(value, axis, step):
    size = lax.axis_size(axis)
    return lax.ppermute(value, axis, [(i, (i + step) % size) for i in range(size)])


def from_partner(value, axis, distance):
    return lax.ppermute(value, axis, [(i, i ^ distance) for i in range(lax.axis_size(axis))])


def two_terms(values):
    top = lax.reduce_precision(values, 8, 7)
    return jnp.concatenate([top, values - top], axis=0).astype(BF16)


def rearranged(grm):
    n_y, n_c, n_z, n_x = (lax.axis_size(name) for name in HI_LO)
    rows = grm.shape[2]
    me_x, me_c = lax.axis_index("x"), lax.axis_index("c")
    blocks = grm.reshape(n_y, n_c, rows, n_z, n_x, rows).transpose(4, 1, 0, 2, 3, 5)
    blocks = blocks.reshape(n_x, n_c, n_y, rows, n_z * rows)
    mine = jnp.zeros_like(blocks)
    for step in range(n_x):
        sent = lax.dynamic_index_in_dim(blocks, (me_x + step) % n_x, 0, keepdims=True)
        arrived = shifted(sent, "x", step) if step else sent
        mine = lax.dynamic_update_slice_in_dim(mine, arrived, (me_x - step) % n_x, axis=0)
    kept = lax.dynamic_index_in_dim(mine, me_c, 1, keepdims=False)
    other = lax.dynamic_index_in_dim(mine, 1 - me_c, 1, keepdims=False)
    both = jnp.concatenate([kept, shifted(other, "c", 1)], axis=-1)
    return both.transpose(1, 0, 2, 3).reshape(n_y * n_x * rows, n_c * n_z * rows)


def local(grm, right_sides, inv_diag, bases, couplings, level_map, variance, iters_per_column):
    rows, rhs = right_sides.shape
    levels = couplings.shape[0] - 1
    rank = couplings.shape[1]
    split_at = levels * rank
    width = rhs + rank
    n_rows, n_columns = lax.axis_size(ROWS), lax.axis_size(COLUMNS)
    me_rows, me_columns = lax.axis_index(ROWS), lax.axis_index(COLUMNS)
    genetic, noise = variance[0], variance[1]

    old = lax.broadcasted_iota(jnp.int32, (split_at, split_at), 0)
    new = jnp.repeat(level_map, rank) * rank + jnp.arange(split_at, dtype=jnp.int32) % rank
    shuffle = (old == new[None, :]).astype(F32)
    by_bit = mm(bases[:, :split_at], shuffle)
    coarse_basis = bases[:, split_at:]

    scale = 1.0 / (n_rows * n_columns * jnp.max(jnp.abs(couplings)))
    couplings = couplings * scale
    diag = (inv_diag * scale)[:, None]
    coarse_coupling = couplings[levels]
    column = lax.broadcasted_iota(jnp.int32, (split_at, split_at), 1)
    repeat = (
        lax.broadcasted_iota(jnp.int32, (rank, split_at), 0)
        == lax.broadcasted_iota(jnp.int32, (rank, split_at), 1) % rank
    )
    tiled = mm(couplings[:levels].reshape(split_at, rank), repeat.astype(F32))
    old_rows = lax.broadcasted_iota(jnp.int32, (split_at, split_at), 0)
    diagonal_blocks = jnp.where(old_rows // rank == column // rank, tiled, 0.0)
    lift = mm(mm(bases[:, :split_at], diagonal_blocks), shuffle)
    lift_terms = two_terms(lift)

    def precondition(field):
        coefficients = tmm(by_bit, field)
        sent = coefficients.astype(BF16).reshape(levels, rank, -1)
        far = [("x", 1), ("x", 2), ("z", 1), ("z", 2), ("z", 4), ("c", 1), ("y", 1), ("y", 2)]
        order = [5, 0, 6, 2, 1, 7, 3, 4]
        arrived = {bit: from_partner(sent[bit], *far[bit]) for bit in order}
        arrived = jnp.concatenate([arrived[bit] for bit in range(levels)], axis=0)
        own = diag * field + mm(lift, coefficients)
        terms = jnp.dot(lift_terms, arrived, preferred_element_type=F32)
        return own + (terms[:rows] + terms[rows:])

    g_block = rearranged(grm)
    own_rows = lax.dynamic_slice_in_dim(g_block, me_rows * rows, rows, axis=0)

    def gathered(block):
        near = from_everyone(block, "z")
        return jnp.stack([near, shifted(near, "c", 1)])

    def image_of(everyone, field, riders=None):
        everyone = everyone.reshape(-1, width)
        partial = jnp.dot(g_block, everyone, preferred_element_type=F32).astype(BF16)
        partial = partial.reshape(n_rows, rows, width)
        if riders is not None:
            riders = jnp.broadcast_to(riders, (n_rows, *riders.shape))
            partial = jnp.concatenate([partial, riders], axis=1)
        arrived = exchanged(partial, ROWS)
        own = jnp.dot(own_rows, everyone, preferred_element_type=F32)
        others = jnp.where(
            jnp.arange(n_rows)[:, None, None] == me_rows,
            jnp.zeros((), F32),
            arrived[:, :rows].astype(F32),
        ).sum(axis=0)
        image = genetic * (own + others) + noise * field
        if riders is None:
            return image
        rode = arrived[:, rows:].astype(F32).sum(axis=0)
        return image, rode[: rode.shape[0] // 2] + rode[rode.shape[0] // 2 :]

    share = rank // n_columns
    parts = tmm(coarse_basis, right_sides).reshape(n_columns, share, rhs)
    t0_rows = exchanged(parts, COLUMNS).sum(axis=0)

    first = jnp.concatenate([precondition(right_sides), coarse_basis], axis=1)
    all_first = gathered(first.astype(BF16))
    first_image = image_of(all_first, first)

    second = precondition(first_image)
    coarse_image = first_image[:, rhs:]
    all_second = gathered(jnp.concatenate([second, coarse_image], axis=1).astype(BF16))
    all_coarse_image = all_second[..., width:].reshape(-1, rank)
    all_second = all_second[..., :width]

    def coarse_rows(everyone):
        whole = lax.dot_general(
            all_coarse_image,
            everyone.reshape(-1, width),
            (((0,), (0,)), ((), ())),
            preferred_element_type=F32,
        )
        return lax.dynamic_slice_in_dim(whole, me_columns * share, share, axis=0)

    t0_rows = jnp.pad(t0_rows, ((0, 0), (0, rank)))
    riders = jnp.concatenate([t0_rows, coarse_rows(all_first), coarse_rows(all_second)], axis=0)
    second_image, riders = image_of(all_second, second, two_terms(riders))

    third = precondition(second_image)
    all_third = gathered(jnp.concatenate([third.astype(BF16), two_terms(riders)], axis=0))
    table = all_third[:, :, rows:].astype(F32)
    table = table[:, :, : 3 * share] + table[:, :, 3 * share :]
    table = jnp.where(lax.axis_index("c") == 0, table, table[::-1])
    table = table.reshape(n_columns, 3, share, width).transpose(1, 0, 2, 3)
    t0, k_first, k_second = table.reshape(3, rank, width)
    third_image = image_of(all_third[:, :, :rows], third)

    k_basis = k_first[:, rhs:]
    s0 = mm(coarse_coupling, t0[:, :rhs])
    s1 = mm(coarse_coupling, k_first[:, :rhs] + mm(k_basis, s0))
    s2 = mm(coarse_coupling, k_second[:, :rhs] + mm(k_second[:, rhs:], s0) + mm(k_basis, s1))
    weights = jnp.concatenate([s0, s1, s2], axis=0)

    none = jnp.zeros_like(coarse_basis)
    coarse_parts = jnp.concatenate(
        [
            jnp.concatenate([coarse_basis, none, none], axis=1),
            jnp.concatenate([second[:, rhs:], coarse_basis, none], axis=1),
            jnp.concatenate([third[:, rhs:], second[:, rhs:], coarse_basis], axis=1),
            jnp.concatenate([coarse_image, none, none], axis=1),
            jnp.concatenate([second_image[:, rhs:], coarse_image, none], axis=1),
        ],
        axis=0,
    )
    coarse_parts = mm(coarse_parts, weights).reshape(5, rows, rhs)
    v = [field[:, :rhs] + coarse_parts[k] for k, field in enumerate([first, second, third])]
    w = [right_sides]
    w += [field[:, :rhs] + coarse_parts[3 + k] for k, field in enumerate([first_image, second_image])]
    last_parts = [third_image[:, rhs:], second_image[:, rhs:], coarse_image]
    w.append(third_image[:, :rhs] + mm(jnp.concatenate(last_parts, axis=1), weights))

    moments = jnp.stack([jnp.sum(w[k - k // 2] * v[k // 2], axis=0) for k in range(2 * STEPS)])
    moments = from_everyone(moments, ROWS).sum(axis=0)
    moments = from_everyone(moments, COLUMNS).sum(axis=0)

    m = [moments[k] for k in range(2 * STEPS)]
    one, zero = jnp.ones_like(m[0]), jnp.zeros_like(m[0])
    in_r, kept_r, kept_x, direction, energy = [one], [one], [], [], None
    for step in range(STEPS):
        basis = range(step + 1)
        fresh = sum(in_r[p] * in_r[q] * m[p + q] for p in basis for q in basis)
        before = [fresh / energy * d for d in direction] if step else []
        direction = [r + d for r, d in zip(in_r, before + [zero])]
        energy = fresh
        alpha = energy / sum(direction[p] * direction[q] * m[p + q + 1] for p in basis for q in basis)
        in_r = [a - b for a, b in zip(in_r + [zero], [zero] + [alpha * d for d in direction])]
        active = step < iters_per_column
        kept_r = [jnp.where(active, a, b) for a, b in zip(in_r, kept_r + [zero])]
        kept_x = [jnp.where(active, b + alpha * d, b) for d, b in zip(direction, kept_x + [zero])]

    solution = sum(c * field for c, field in zip(kept_x, v))
    residual = w[0] + sum(c * field for c, field in zip(kept_r[1:], w[1:]))
    return (solution, residual)


def solution(mesh):
    split = Mesh(mesh.devices.reshape(4, 2, 8, 4), HI_LO)
    return jax.shard_map(
        local,
        mesh=split,
        in_specs=(
            P(None, LO, None, HI, None),
            P(HI_LO, None),
            P(HI_LO),
            P(HI_LO, None),
            P(),
            P(),
            P(),
            P(),
        ),
        out_specs=(P(HI_LO, None), P(HI_LO, None)),
        check_vma=False,
    )
```

```python
import functools

import jax
import jax.numpy as jnp
from jax import lax
from jax.experimental import pallas as pl
from jax.experimental.pallas import tpu as pltpu
from jax.sharding import Mesh
from jax.sharding import PartitionSpec as P


HI = ("y", "c")
LO = ("z", "x")
HI_LO = ("y", "c", "z", "x")
COLUMNS = ("c", "z")
ROWS = ("y", "x")
BF16 = jnp.bfloat16
F32 = jnp.float32
EXACT = lax.Precision.HIGHEST
STEPS = 3
INTERPRET = False


def mm(left, right):
    return jnp.dot(left, right, precision=EXACT)


def tmm(left, right):
    return lax.dot_general(left, right, (((0,), (0,)), ((), ())), precision=EXACT)


def from_everyone(array, axes):
    copies = jnp.broadcast_to(array, (lax.axis_size(axes), *array.shape))
    return lax.all_to_all(copies, axes, split_axis=0, concat_axis=0, tiled=True)


def exchanged(array, axes):
    return lax.all_to_all(array, axes, split_axis=0, concat_axis=0, tiled=True)


def shifted(value, axis, step):
    size = lax.axis_size(axis)
    return lax.ppermute(value, axis, [(i, (i + step) % size) for i in range(size)])


def from_partner(value, axis, distance):
    return lax.ppermute(value, axis, [(i, i ^ distance) for i in range(lax.axis_size(axis))])


def two_terms(values):
    top = lax.reduce_precision(values, 8, 7)
    return jnp.concatenate([top, values - top], axis=0).astype(BF16)


def by_x_kernel(n_x, n_z, n_c, me_ref, grm_ref, out_ref):
    rows = grm_ref.shape[1]
    me_x, me_c = me_ref[0], me_ref[1]
    for block in range(grm_ref.shape[0]):
        whole = grm_ref[block]
        y, c = divmod(block, n_c)
        for x in range(n_x):
            starts = [(z * n_x + x) * rows for z in range(n_z)]
            columns = jnp.concatenate([whole[:, at : at + rows] for at in starts], axis=1)
            out_ref[lax.rem(x - me_x + n_x, n_x), lax.rem(c + me_c, n_c), y] = columns


def rearranged(grm):
    n_y, n_c, n_z, n_x = (lax.axis_size(name) for name in HI_LO)
    rows = grm.shape[2]
    me_x, me_c = lax.axis_index("x"), lax.axis_index("c")
    blocks = pl.pallas_call(
        functools.partial(by_x_kernel, n_x, n_z, n_c),
        out_shape=jax.ShapeDtypeStruct((n_x, n_c, n_y, rows, n_z * rows), grm.dtype),
        in_specs=[
            pl.BlockSpec(memory_space=pltpu.SMEM),
            pl.BlockSpec(memory_space=pltpu.VMEM),
        ],
        out_specs=pl.BlockSpec(memory_space=pltpu.VMEM),
        name="by_x",
        interpret=INTERPRET,
    )(jnp.stack([me_x, me_c]).astype(jnp.int32), grm.reshape(n_y * n_c, rows, n_z * n_x * rows))
    mine = jnp.zeros_like(blocks)
    for step in range(n_x):
        arrived = shifted(blocks[step : step + 1], "x", step) if step else blocks[:1]
        mine = lax.dynamic_update_slice_in_dim(mine, arrived, (me_x - step) % n_x, axis=0)
    both = jnp.concatenate([mine[:, 0], shifted(mine[:, 1], "c", 1)], axis=-1)
    return both.transpose(1, 0, 2, 3).reshape(n_y * n_x * rows, n_c * n_z * rows)


def lift_kernel(levels, width, own_ref, lift_ref, *refs):
    arrived, (out_ref, sent_ref) = refs[:levels], refs[-2:]
    rank = arrived[0].shape[0]
    rows = own_ref.shape[0]
    terms = sum(
        jnp.dot(
            lift_ref[:, bit * rank : (bit + 1) * rank],
            arrived[bit][...],
            preferred_element_type=F32,
        )
        for bit in range(levels)
    )
    field = own_ref[...] + (terms[:rows] + terms[rows:])
    out_ref[...] = field
    whole = field.astype(BF16)
    extra = refs[levels:-2]
    beside = [ref for ref in extra if ref.shape[0] == rows]
    below = [ref for ref in extra if ref.shape[0] != rows]
    if beside:
        whole = jnp.concatenate([whole] + [ref[...].astype(BF16) for ref in beside], axis=1)
    for copy in range(sent_ref.shape[0]):
        sent_ref[copy, :rows] = whole
        for ref in below:
            sent_ref[copy, rows:] = ref[...]


def local(grm, right_sides, inv_diag, bases, couplings, level_map, variance, iters_per_column):
    rows, rhs = right_sides.shape
    levels = couplings.shape[0] - 1
    rank = couplings.shape[1]
    split_at = levels * rank
    width = rhs + rank
    n_rows, n_columns = lax.axis_size(ROWS), lax.axis_size(COLUMNS)
    me_rows, me_columns = lax.axis_index(ROWS), lax.axis_index(COLUMNS)
    genetic, noise = variance[0], variance[1]

    old = lax.broadcasted_iota(jnp.int32, (split_at, split_at), 0)
    new = jnp.repeat(level_map, rank) * rank + jnp.arange(split_at, dtype=jnp.int32) % rank
    shuffle = (old == new[None, :]).astype(F32)
    by_bit = mm(bases[:, :split_at], shuffle)
    coarse_basis = bases[:, split_at:]

    scale = 1.0 / (n_rows * n_columns * jnp.max(jnp.abs(couplings)))
    couplings = couplings * scale
    diag = (inv_diag * scale)[:, None]
    coarse_coupling = couplings[levels]
    column = lax.broadcasted_iota(jnp.int32, (split_at, split_at), 1)
    repeat = (
        lax.broadcasted_iota(jnp.int32, (rank, split_at), 0)
        == lax.broadcasted_iota(jnp.int32, (rank, split_at), 1) % rank
    )
    tiled = mm(couplings[:levels].reshape(split_at, rank), repeat.astype(F32))
    old_rows = lax.broadcasted_iota(jnp.int32, (split_at, split_at), 0)
    diagonal_blocks = jnp.where(old_rows // rank == column // rank, tiled, 0.0)
    lift = mm(mm(bases[:, :split_at], diagonal_blocks), shuffle)
    lift_terms = two_terms(lift)

    def precondition(field, beside=None, below=None):
        coefficients = tmm(by_bit, field)
        sent = coefficients.astype(BF16).reshape(levels, rank, -1)
        far = [("x", 1), ("x", 2), ("z", 1), ("z", 2), ("z", 4), ("c", 1), ("y", 1), ("y", 2)]
        order = [5, 0, 6, 2, 1, 7, 3, 4]
        arrived = {bit: from_partner(sent[bit], *far[bit]) for bit in order}
        own = diag * field + mm(lift, coefficients)
        extra = [array for array in (beside, below) if array is not None]
        more_rows = 0 if below is None else below.shape[0]
        more_columns = 0 if beside is None else beside.shape[1]
        sent_shape = (lax.axis_size("z"), rows + more_rows, own.shape[1] + more_columns)
        return pl.pallas_call(
            functools.partial(lift_kernel, levels, width),
            out_shape=(
                jax.ShapeDtypeStruct(own.shape, F32),
                jax.ShapeDtypeStruct(sent_shape, BF16),
            ),
            name="lift",
            interpret=INTERPRET,
        )(own, lift_terms, *[arrived[bit] for bit in range(levels)], *extra)

    g_block = rearranged(grm)
    own_rows = lax.dynamic_slice_in_dim(g_block, me_rows * rows, rows, axis=0)

    def gathered(copies):
        near = exchanged(copies, "z")
        return near, shifted(near, "c", 1)

    def times(block, everyone):
        near, far = (half.reshape(-1, width) for half in everyone)
        depth = near.shape[0]
        product = jnp.dot(block[:, :depth], near, preferred_element_type=F32)
        return product + jnp.dot(block[:, depth:], far, preferred_element_type=F32)

    def image_of(everyone, field, riders=None):
        partial = times(g_block, everyone).astype(BF16).reshape(n_rows, rows, width)
        if riders is not None:
            partial = jnp.concatenate([partial, riders], axis=1)
        arrived = exchanged(partial, ROWS)
        own = times(own_rows, everyone)
        others = jnp.where(
            jnp.arange(n_rows)[:, None, None] == me_rows,
            jnp.zeros((), F32),
            arrived[:, :rows].astype(F32),
        ).sum(axis=0)
        return genetic * (own + others) + noise * field, arrived[:, rows:]

    def sum_of_terms(terms, axis):
        top, rest = jnp.split(terms.astype(F32), 2, axis=axis)
        return top + rest

    def for_everyone(array):
        return jnp.broadcast_to(array, (n_rows, *array.shape))

    share = rank // n_columns
    t_share = rank // n_rows
    t_parts = tmm(coarse_basis, right_sides).reshape(n_rows, t_share, rhs)
    t_parts = jnp.pad(t_parts, ((0, 0), (0, 0), (0, rank)))
    t_top = lax.reduce_precision(t_parts, 8, 7)
    t_parts = jnp.concatenate([t_top, t_parts - t_top], axis=1).astype(BF16)

    first, copies = precondition(right_sides, beside=coarse_basis)
    first = jnp.concatenate([first, coarse_basis], axis=1)
    all_first = gathered(copies)
    first_image, rode = image_of(all_first, first, t_parts)
    t_rows = sum_of_terms(rode, 1).sum(axis=0)
    t_rows = jnp.concatenate([t_rows, jnp.zeros((t_share, rank), F32)], axis=1)

    coarse_image = first_image[:, rhs:]
    second, copies = precondition(first_image, beside=coarse_image, below=two_terms(t_rows))
    all_second = gathered(copies)
    all_coarse_image = [half[:, :rows, width:].reshape(-1, rank) for half in all_second]
    t_rows = sum(sum_of_terms(half[:, rows:, :width], 1).sum(axis=0) for half in all_second)
    all_second = [half[:, :rows, :width] for half in all_second]

    def coarse_rows(everyone):
        whole = sum(
            lax.dot_general(
                image,
                half.reshape(-1, width),
                (((0,), (0,)), ((), ())),
                preferred_element_type=F32,
            )
            for image, half in zip(all_coarse_image, everyone)
        )
        return lax.dynamic_slice_in_dim(whole, me_columns * share, share, axis=0)

    riders = jnp.concatenate([t_rows, coarse_rows(all_first), coarse_rows(all_second)], axis=0)
    second_image, rode = image_of(all_second, second, for_everyone(two_terms(riders)))
    rode = sum_of_terms(rode, 1)
    t0 = rode[:, :t_share].reshape(rank, width)

    third, copies = precondition(second_image, below=two_terms(rode[:, t_share:].sum(axis=0)))
    all_third = gathered(copies)
    table = sum_of_terms(jnp.stack([half[:, rows:] for half in all_third]), 2)
    table = jnp.where(lax.axis_index("c") == 0, table, table[::-1])
    table = table.reshape(n_columns, 2, share, width).transpose(1, 0, 2, 3)
    k_first, k_second = table.reshape(2, rank, width)
    third_image, _ = image_of([half[:, :rows] for half in all_third], third)

    k_basis = k_first[:, rhs:]
    s0 = mm(coarse_coupling, t0[:, :rhs])
    s1 = mm(coarse_coupling, k_first[:, :rhs] + mm(k_basis, s0))
    s2 = mm(coarse_coupling, k_second[:, :rhs] + mm(k_second[:, rhs:], s0) + mm(k_basis, s1))
    weights = jnp.concatenate([s0, s1, s2], axis=0)

    none = jnp.zeros_like(coarse_basis)
    coarse_parts = jnp.concatenate(
        [
            jnp.concatenate([coarse_basis, none, none], axis=1),
            jnp.concatenate([second[:, rhs:], coarse_basis, none], axis=1),
            jnp.concatenate([third[:, rhs:], second[:, rhs:], coarse_basis], axis=1),
            jnp.concatenate([coarse_image, none, none], axis=1),
            jnp.concatenate([second_image[:, rhs:], coarse_image, none], axis=1),
        ],
        axis=0,
    )
    coarse_parts = mm(coarse_parts, weights).reshape(5, rows, rhs)
    v = [field[:, :rhs] + coarse_parts[k] for k, field in enumerate([first, second, third])]
    w = [right_sides]
    w += [field[:, :rhs] + coarse_parts[3 + k] for k, field in enumerate([first_image, second_image])]
    last_parts = [third_image[:, rhs:], second_image[:, rhs:], coarse_image]
    w.append(third_image[:, :rhs] + mm(jnp.concatenate(last_parts, axis=1), weights))

    moments = jnp.stack([jnp.sum(w[k - k // 2] * v[k // 2], axis=0) for k in range(2 * STEPS)])
    moments = from_everyone(moments, ROWS).sum(axis=0)
    moments = from_everyone(moments, COLUMNS).sum(axis=0)

    m = [moments[k] for k in range(2 * STEPS)]
    one, zero = jnp.ones_like(m[0]), jnp.zeros_like(m[0])
    in_r, kept_r, kept_x, direction, energy = [one], [one], [], [], None
    for step in range(STEPS):
        basis = range(step + 1)
        fresh = sum(in_r[p] * in_r[q] * m[p + q] for p in basis for q in basis)
        before = [fresh / energy * d for d in direction] if step else []
        direction = [r + d for r, d in zip(in_r, before + [zero])]
        energy = fresh
        alpha = energy / sum(direction[p] * direction[q] * m[p + q + 1] for p in basis for q in basis)
        in_r = [a - b for a, b in zip(in_r + [zero], [zero] + [alpha * d for d in direction])]
        active = step < iters_per_column
        kept_r = [jnp.where(active, a, b) for a, b in zip(in_r, kept_r + [zero])]
        kept_x = [jnp.where(active, b + alpha * d, b) for d, b in zip(direction, kept_x + [zero])]

    solution = sum(c * field for c, field in zip(kept_x, v))
    residual = w[0] + sum(c * field for c, field in zip(kept_r[1:], w[1:]))
    return (solution, residual)


def solution(mesh):
    split = Mesh(mesh.devices.reshape(4, 2, 8, 4), HI_LO)
    return jax.shard_map(
        local,
        mesh=split,
        in_specs=(
            P(None, LO, None, HI, None),
            P(HI_LO, None),
            P(HI_LO),
            P(HI_LO, None),
            P(),
            P(),
            P(),
            P(),
        ),
        out_specs=(P(HI_LO, None), P(HI_LO, None)),
        check_vma=False,
    )
```

```python
import functools

import jax
import jax.numpy as jnp
from jax import lax
from jax.experimental import pallas as pl
from jax.experimental.pallas import tpu as pltpu
from jax.sharding import Mesh
from jax.sharding import PartitionSpec as P


HI = ("y", "c")
LO = ("z", "x")
HI_LO = ("y", "c", "z", "x")
COLUMNS = ("c", "z")
ROWS = ("y", "x")
BF16 = jnp.bfloat16
F32 = jnp.float32
EXACT = lax.Precision.HIGHEST
STEPS = 3
INTERPRET = False


def mm(left, right):
    return jnp.dot(left, right, precision=EXACT)


def mm3(left, right):
    return jnp.dot(left, right, precision=lax.Precision.HIGH)


def from_everyone(array, axes):
    copies = jnp.broadcast_to(array, (lax.axis_size(axes), *array.shape))
    return lax.all_to_all(copies, axes, split_axis=0, concat_axis=0, tiled=True)


def exchanged(array, axes):
    return lax.all_to_all(array, axes, split_axis=0, concat_axis=0, tiled=True)


def shifted(value, axis, step):
    size = lax.axis_size(axis)
    return lax.ppermute(value, axis, [(i, (i + step) % size) for i in range(size)])


def from_partner(value, axis, distance):
    return lax.ppermute(value, axis, [(i, i ^ distance) for i in range(lax.axis_size(axis))])


def two_terms(values):
    top = lax.reduce_precision(values, 8, 7)
    return jnp.concatenate([top, values - top], axis=0).astype(BF16)


def by_x_kernel(n_x, n_z, n_c, me_ref, grm_ref, out_ref):
    rows = grm_ref.shape[1]
    me_x, me_c = me_ref[0], me_ref[1]

    def regroup(block, _):
        whole = grm_ref[block]
        y, c = lax.div(block, n_c), lax.rem(block, n_c)
        for x in range(n_x):
            starts = [(z * n_x + x) * rows for z in range(n_z)]
            columns = jnp.concatenate([whole[:, at : at + rows] for at in starts], axis=1)
            out_ref[lax.rem(x - me_x + n_x, n_x), lax.rem(c + me_c, n_c), y] = columns
        return 0

    lax.fori_loop(0, grm_ref.shape[0], regroup, 0)


def rearranged(grm):
    n_y, n_c, n_z, n_x = (lax.axis_size(name) for name in HI_LO)
    rows = grm.shape[2]
    me_x, me_c = lax.axis_index("x"), lax.axis_index("c")
    blocks = pl.pallas_call(
        functools.partial(by_x_kernel, n_x, n_z, n_c),
        out_shape=jax.ShapeDtypeStruct((n_x, n_c, n_y, rows, n_z * rows), grm.dtype),
        in_specs=[
            pl.BlockSpec(memory_space=pltpu.SMEM),
            pl.BlockSpec(memory_space=pltpu.VMEM),
        ],
        out_specs=pl.BlockSpec(memory_space=pltpu.VMEM),
        name="by_x",
        interpret=INTERPRET,
    )(jnp.stack([me_x, me_c]).astype(jnp.int32), grm.reshape(n_y * n_c, rows, n_z * n_x * rows))
    mine = jnp.zeros_like(blocks)
    for step in range(n_x):
        arrived = shifted(blocks[step : step + 1], "x", step) if step else blocks[:1]
        mine = lax.dynamic_update_slice_in_dim(mine, arrived, (me_x - step) % n_x, axis=0)
    both = jnp.concatenate([mine[:, 0], shifted(mine[:, 1], "c", 1)], axis=-1)
    return both.transpose(1, 0, 2, 3).reshape(n_y * n_x * rows, n_c * n_z * rows)


def times_kernel(rows, width, n_terms, me_ref, g_ref, near_ref, far_ref, *refs):
    out_ref, own_ref, field_ref = refs[-4:-1] if n_terms else refs[-3:]
    at = 0
    for half in (near_ref, far_ref):
        for z in range(half.shape[0]):
            field_ref[at : at + rows] = half[z, :rows, :width]
            at += rows
    per_step = 4

    def multiply(step, _):
        first = step * per_step
        product = jnp.dot(
            g_ref[pl.ds(pl.multiple_of(first * rows, per_step * rows), per_step * rows)],
            field_ref[...],
            preferred_element_type=F32,
        )
        for k in range(per_step):
            block = product[k * rows : (k + 1) * rows]
            out_ref[first + k, :rows] = block.astype(BF16)

            @pl.when(me_ref[0] == first + k)
            def _():
                own_ref[...] = block

        return 0

    lax.fori_loop(0, out_ref.shape[0] // per_step, multiply, 0)
    if n_terms:
        t_ref, near_first_ref, far_first_ref = refs[:3]
        rider_ref = refs[-1]
        share = t_ref.shape[0]
        rank = near_ref.shape[2] - width
        depth = near_ref.shape[0] * rows
        rider_ref[:share] = t_ref[...]
        for k, pair in enumerate([(near_first_ref, far_first_ref), None]):
            total = None
            for i, half in enumerate((near_ref, far_ref)):
                image = half[:, :rows, width:].reshape(depth, rank)
                if pair:
                    other = pair[i][:, :, :width].reshape(depth, width)
                else:
                    other = field_ref[i * depth : (i + 1) * depth]
                part = lax.dot_general(
                    image, other, (((0,), (0,)), ((), ())), preferred_element_type=F32
                )
                total = part if total is None else total + part
            mine = jnp.zeros((share, width), F32)
            for i in range(rank // share):
                mine = jnp.where(me_ref[1] == i, total[i * share : (i + 1) * share], mine)
            rider_ref[(k + 1) * share : (k + 2) * share] = mine
        values = rider_ref[...]
        top = values.astype(BF16)
        rest = (values - top.astype(F32)).astype(BF16)
        below = jnp.concatenate([top, rest], axis=0)
        for d in range(out_ref.shape[0]):
            out_ref[d, rows:] = below
    elif out_ref.shape[1] > rows:
        for d in range(out_ref.shape[0]):
            out_ref[d, rows:] = refs[0][d]


def in_two(values):
    top = values.astype(BF16)
    return top, (values - top.astype(F32)).astype(BF16)


def send_coefficients(field, basis_ref, sent_refs):
    top, rest = in_two(field)
    terms = jnp.concatenate([top, rest, top], axis=0)
    coefficients = jnp.dot(basis_ref[...], terms, preferred_element_type=F32).astype(BF16)
    rank = sent_refs[0].shape[0]
    for bit, ref in enumerate(sent_refs):
        ref[...] = coefficients[bit * rank : (bit + 1) * rank]


def coefficients_kernel(field_ref, basis_ref, *sent_refs):
    send_coefficients(field_ref[...], basis_ref, sent_refs)


def image_kernel(me_ref, variance_ref, arrived_ref, own_ref, field_ref, *refs):
    rows = own_ref.shape[0]

    def add(d, total):
        part = arrived_ref[d, :rows].astype(F32)
        return total + jnp.where(me_ref[0] == d, jnp.zeros_like(part), part)

    total = lax.fori_loop(0, arrived_ref.shape[0], add, own_ref[...])
    image = variance_ref[0] * total + variance_ref[1] * field_ref[...]
    if len(refs) == 1:
        refs[0][...] = image
    else:
        refs[1][...] = image
        send_coefficients(image, refs[0], refs[2:])


def lift_kernel(levels, field_ref, own_ref, lift_ref, *refs):
    arrived, (out_ref, sent_ref) = refs[:levels], refs[-2:]
    rank = arrived[0].shape[0]
    rows = field_ref.shape[0]
    terms = sum(
        jnp.dot(
            lift_ref[:, bit * rank : (bit + 1) * rank],
            arrived[bit][...],
            preferred_element_type=F32,
        )
        for bit in range(levels)
    )
    field = jnp.dot(own_ref[...], field_ref[...], precision=EXACT, preferred_element_type=F32)
    field = field + (terms[:rows] + terms[rows:])
    out_ref[...] = field
    whole = field.astype(BF16)
    extra = refs[levels:-2]
    beside = [ref for ref in extra if ref.shape[0] == rows]
    below = [ref for ref in extra if ref.shape[0] != rows]
    if beside:
        whole = jnp.concatenate([whole] + [ref[...].astype(BF16) for ref in beside], axis=1)
    for copy in range(sent_ref.shape[0]):
        sent_ref[copy, :rows] = whole
        for ref in below:
            sent_ref[copy, rows:] = ref[...]


def kernel_call(kernel, name, shapes, operands, scalars=0, scratch=()):
    in_smem = [pl.BlockSpec(memory_space=pltpu.SMEM)] * scalars
    in_vmem = [pl.BlockSpec(memory_space=pltpu.VMEM)] * (len(operands) - scalars)
    return pl.pallas_call(
        kernel,
        out_shape=[jax.ShapeDtypeStruct(shape, dtype) for shape, dtype in shapes],
        in_specs=in_smem + in_vmem,
        out_specs=[pl.BlockSpec(memory_space=pltpu.VMEM)] * len(shapes),
        scratch_shapes=[pltpu.VMEM(shape, dtype) for shape, dtype in scratch],
        name=name,
        interpret=INTERPRET,
    )(*operands)


def local(grm, right_sides, inv_diag, bases, couplings, level_map, variance, iters_per_column):
    rows, rhs = right_sides.shape
    levels = couplings.shape[0] - 1
    rank = couplings.shape[1]
    split_at = levels * rank
    width = rhs + rank
    n_rows, n_columns = lax.axis_size(ROWS), lax.axis_size(COLUMNS)
    me_rows, me_columns = lax.axis_index(ROWS), lax.axis_index(COLUMNS)

    old = lax.broadcasted_iota(jnp.int32, (split_at, split_at), 0)
    new = jnp.repeat(level_map, rank) * rank + jnp.arange(split_at, dtype=jnp.int32) % rank
    shuffle = (old == new[None, :]).astype(F32)
    by_bit = mm3(bases[:, :split_at], shuffle)
    coarse_basis = bases[:, split_at:]

    scale = 1.0 / (n_rows * n_columns * jnp.max(jnp.abs(couplings)))
    couplings = couplings * scale
    diag = (inv_diag * scale)[:, None]
    coarse_coupling = couplings[levels]
    column = lax.broadcasted_iota(jnp.int32, (split_at, split_at), 1)
    repeat = (
        lax.broadcasted_iota(jnp.int32, (rank, split_at), 0)
        == lax.broadcasted_iota(jnp.int32, (rank, split_at), 1) % rank
    )
    tiled = mm3(couplings[:levels].reshape(split_at, rank), repeat.astype(F32))
    old_rows = lax.broadcasted_iota(jnp.int32, (split_at, split_at), 0)
    diagonal_blocks = jnp.where(old_rows // rank == column // rank, tiled, 0.0)
    lift = mm3(mm3(bases[:, :split_at], diagonal_blocks), shuffle)
    lift_terms = two_terms(lift)
    eye = lax.broadcasted_iota(jnp.int32, (rows, rows), 0) == jnp.arange(rows)[None]
    own_lift = mm3(lift, by_bit.T) + jnp.where(eye, diag, 0.0)
    basis_top, basis_rest = jnp.split(two_terms(by_bit.T), 2, axis=0)
    basis_terms = jnp.concatenate([basis_top, basis_top, basis_rest], axis=1)

    def coefficient_shapes(columns):
        return [((rank, columns), BF16)] * levels

    def precondition(field, sent, beside=None, below=None):
        far = [("x", 1), ("x", 2), ("z", 1), ("z", 2), ("z", 4), ("c", 1), ("y", 1), ("y", 2)]
        order = [5, 0, 6, 2, 1, 7, 3, 4]
        arrived = {bit: from_partner(sent[bit], *far[bit]) for bit in order}
        extra = [array for array in (beside, below) if array is not None]
        more_rows = 0 if below is None else below.shape[0]
        more_columns = 0 if beside is None else beside.shape[1]
        columns = field.shape[1]
        sent_shape = (lax.axis_size("z"), rows + more_rows, columns + more_columns)
        return kernel_call(
            functools.partial(lift_kernel, levels),
            "lift",
            [((rows, columns), F32), (sent_shape, BF16)],
            [field, own_lift, lift_terms, *[arrived[bit] for bit in range(levels)], *extra],
        )

    places = jnp.stack([me_rows, me_columns]).astype(jnp.int32)
    sent = kernel_call(
        coefficients_kernel, "coefficients", coefficient_shapes(rhs), [right_sides, basis_terms]
    )
    grm, *sent = lax.optimization_barrier((grm, *sent))
    g_block = rearranged(grm)

    def gathered(copies):
        near = exchanged(copies, "z")
        return near, shifted(near, "c", 1)

    def products(everyone, riders=None, more_rows=0, n_terms=0):
        shapes = [((n_rows, rows + more_rows, width), BF16), ((rows, width), F32)]
        scratch = [((n_columns * rows, width), BF16)]
        if n_terms:
            scratch.append(((more_rows // 2, width), F32))
        partial, own = kernel_call(
            functools.partial(times_kernel, rows, width, n_terms),
            "times",
            shapes,
            [places, g_block, *everyone, *([] if riders is None else riders)],
            1,
            scratch,
        )
        return exchanged(partial, ROWS), own

    def image_of(arrived, own, field, send=True):
        shapes = [((rows, width), F32)] + (coefficient_shapes(width) if send else [])
        operands = [places, variance, arrived, own, field] + ([basis_terms] if send else [])
        image, *sent = kernel_call(image_kernel, "image", shapes, operands, 2)
        return image, sent

    def sum_of_terms(terms, axis):
        top, rest = jnp.split(terms.astype(F32), 2, axis=axis)
        return top + rest

    share = rank // n_columns
    t_share = rank // n_rows
    t_parts = mm3(coarse_basis.T, right_sides).reshape(n_rows, t_share, rhs)
    t_parts = jnp.pad(t_parts, ((0, 0), (0, 0), (0, rank)))
    t_top = lax.reduce_precision(t_parts, 8, 7)
    t_parts = jnp.concatenate([t_top, t_parts - t_top], axis=1).astype(BF16)

    first, copies = precondition(right_sides, sent, beside=coarse_basis)
    first = jnp.concatenate([first, coarse_basis], axis=1)
    all_first = gathered(copies)
    arrived, own = products(all_first, [t_parts], t_parts.shape[1])
    first_image, sent = image_of(arrived, own, first)
    t_rows = sum_of_terms(arrived[:, rows:], 1).sum(axis=0)
    t_rows = jnp.concatenate([t_rows, jnp.zeros((t_share, rank), F32)], axis=1)

    coarse_image = first_image[:, rhs:]
    second, copies = precondition(
        first_image, sent, beside=coarse_image, below=two_terms(t_rows)
    )
    all_second = gathered(copies)
    t_rows = sum(sum_of_terms(half[:, rows:, :width], 1).sum(axis=0) for half in all_second)
    arrived, own = products(all_second, [t_rows, *all_first], 6 * share, 2)
    second_image, sent = image_of(arrived, own, second)
    rode = sum_of_terms(arrived[:, rows:], 1)
    t0 = rode[:, :t_share].reshape(rank, width)

    third, copies = precondition(
        second_image, sent, below=two_terms(rode[:, t_share:].sum(axis=0))
    )
    all_third = gathered(copies)
    arrived, own = products(all_third)
    third_image, _ = image_of(arrived, own, third, send=False)
    table = sum_of_terms(jnp.stack([half[:, rows:] for half in all_third]), 2)
    table = jnp.where(lax.axis_index("c") == 0, table, table[::-1])
    table = table.reshape(n_columns, 2, share, width).transpose(1, 0, 2, 3)
    k_first, k_second = table.reshape(2, rank, width)

    k_basis = k_first[:, rhs:]
    s0 = mm(coarse_coupling, t0[:, :rhs])
    s1 = mm(coarse_coupling, k_first[:, :rhs] + mm(k_basis, s0))
    s2 = mm(coarse_coupling, k_second[:, :rhs] + mm(k_second[:, rhs:], s0) + mm(k_basis, s1))
    weights = jnp.concatenate([s0, s1, s2], axis=0)

    none = jnp.zeros_like(coarse_basis)
    coarse_parts = jnp.concatenate(
        [
            jnp.concatenate([coarse_basis, none, none], axis=1),
            jnp.concatenate([second[:, rhs:], coarse_basis, none], axis=1),
            jnp.concatenate([third[:, rhs:], second[:, rhs:], coarse_basis], axis=1),
            jnp.concatenate([coarse_image, none, none], axis=1),
            jnp.concatenate([second_image[:, rhs:], coarse_image, none], axis=1),
        ],
        axis=0,
    )
    coarse_parts = mm3(coarse_parts, weights).reshape(5, rows, rhs)
    v = [field[:, :rhs] + coarse_parts[k] for k, field in enumerate([first, second, third])]
    w = [right_sides]
    w += [field[:, :rhs] + coarse_parts[3 + k] for k, field in enumerate([first_image, second_image])]
    last_parts = [third_image[:, rhs:], second_image[:, rhs:], coarse_image]
    w.append(third_image[:, :rhs] + mm3(jnp.concatenate(last_parts, axis=1), weights))

    moments = jnp.stack([jnp.sum(w[k - k // 2] * v[k // 2], axis=0) for k in range(2 * STEPS)])
    moments = from_everyone(moments, ROWS).sum(axis=0)
    moments = from_everyone(moments, COLUMNS).sum(axis=0)

    m = [moments[k] for k in range(2 * STEPS)]
    one, zero = jnp.ones_like(m[0]), jnp.zeros_like(m[0])
    in_r, kept_r, kept_x, direction, energy = [one], [one], [], [], None
    for step in range(STEPS):
        basis = range(step + 1)
        fresh = sum(in_r[p] * in_r[q] * m[p + q] for p in basis for q in basis)
        before = [fresh / energy * d for d in direction] if step else []
        direction = [r + d for r, d in zip(in_r, before + [zero])]
        energy = fresh
        alpha = energy / sum(direction[p] * direction[q] * m[p + q + 1] for p in basis for q in basis)
        in_r = [a - b for a, b in zip(in_r + [zero], [zero] + [alpha * d for d in direction])]
        active = step < iters_per_column
        kept_r = [jnp.where(active, a, b) for a, b in zip(in_r, kept_r + [zero])]
        kept_x = [jnp.where(active, b + alpha * d, b) for d, b in zip(direction, kept_x + [zero])]

    solution = sum(c * field for c, field in zip(kept_x, v))
    residual = w[0] + sum(c * field for c, field in zip(kept_r[1:], w[1:]))
    return (solution, residual)


def solution(mesh):
    split = Mesh(mesh.devices.reshape(4, 2, 8, 4), HI_LO)
    return jax.shard_map(
        local,
        mesh=split,
        in_specs=(
            P(None, LO, None, HI, None),
            P(HI_LO, None),
            P(HI_LO),
            P(HI_LO, None),
            P(),
            P(),
            P(),
            P(),
        ),
        out_specs=(P(HI_LO, None), P(HI_LO, None)),
        check_vma=False,
    )
```

```python
import functools

import jax
import jax.numpy as jnp
from jax import lax
from jax.experimental import pallas as pl
from jax.experimental.pallas import tpu as pltpu
from jax.sharding import Mesh
from jax.sharding import PartitionSpec as P


HI = ("y", "c")
LO = ("z", "x")
HI_LO = ("y", "c", "z", "x")
COLUMNS = ("c", "z")
ROWS = ("y", "x")
BF16 = jnp.bfloat16
F32 = jnp.float32
EXACT = lax.Precision.HIGHEST
STEPS = 3
INTERPRET = False
PARTS = 1


def mm(left, right):
    return jnp.dot(left, right, precision=EXACT)


def mm3(left, right):
    return jnp.dot(left, right, precision=lax.Precision.HIGH)


def from_everyone(array, axes):
    copies = jnp.broadcast_to(array, (lax.axis_size(axes), *array.shape))
    return lax.all_to_all(copies, axes, split_axis=0, concat_axis=0, tiled=True)


def exchanged(array, axes):
    return lax.all_to_all(array, axes, split_axis=0, concat_axis=0, tiled=True)


def shifted(value, axis, step):
    size = lax.axis_size(axis)
    return lax.ppermute(value, axis, [(i, (i + step) % size) for i in range(size)])


def from_partner(value, axis, distance):
    return lax.ppermute(value, axis, [(i, i ^ distance) for i in range(lax.axis_size(axis))])


def two_terms(values):
    top = lax.reduce_precision(values, 8, 7)
    return jnp.concatenate([top, values - top], axis=0).astype(BF16)


def by_x_kernel(n_x, n_z, me_ref, grm_ref, *out_refs):
    rows = grm_ref.shape[1]
    whole = grm_ref[0]
    for x in range(n_x):
        starts = [(z * n_x + x) * rows for z in range(n_z)]
        columns = jnp.concatenate([whole[:, at : at + rows] for at in starts], axis=1)
        for step, out_ref in enumerate(out_refs):

            @pl.when(lax.rem(x - me_ref[0] + n_x, n_x) == step)
            def _():
                out_ref[0] = columns


def place_kernel(n_x, n_c, me_ref, *refs):
    arrived, (kept_ref, other_ref) = refs[:n_x], refs[n_x:]
    for step, ref in enumerate(arrived):
        x = lax.rem(me_ref[0] - step + n_x, n_x)
        for y in range(ref.shape[0] // n_c):
            kept_ref[y, x] = ref[y * n_c + me_ref[1]]
            other_ref[y, x] = ref[y * n_c + 1 - me_ref[1]]


def cut_by_x(grm):
    n_y, n_c, n_z, n_x = (lax.axis_size(name) for name in HI_LO)
    rows = grm.shape[2]
    me = lax.axis_index("x").astype(jnp.int32)[None]
    depth = n_z * rows
    return pl.pallas_call(
        functools.partial(by_x_kernel, n_x, n_z),
        grid=(n_y * n_c,),
        out_shape=[jax.ShapeDtypeStruct((n_y * n_c, rows, depth), grm.dtype)] * n_x,
        in_specs=[
            pl.BlockSpec(memory_space=pltpu.SMEM),
            pl.BlockSpec((1, rows, n_x * depth), lambda i: (i, 0, 0)),
        ],
        out_specs=[pl.BlockSpec((1, rows, depth), lambda i: (i, 0, 0))] * n_x,
        name="by_x",
        interpret=INTERPRET,
    )(me, grm.reshape(n_y * n_c, rows, n_x * depth))


def rearranged(blocks):
    n_y, n_c, _, n_x = (lax.axis_size(name) for name in HI_LO)
    _, rows, depth = blocks[0].shape
    me = jnp.stack([lax.axis_index("x"), lax.axis_index("c")]).astype(jnp.int32)
    arrived = [shifted(block, "x", k) if k else block for k, block in enumerate(blocks)]
    kept, other = kernel_call(
        functools.partial(place_kernel, n_x, n_c),
        [((n_y, n_x, rows, depth), BF16)] * 2,
        [me, *arrived],
        1,
    )
    return kept.reshape(-1, depth), shifted(other, "c", 1).reshape(-1, depth)


def times_kernel(rows, width, share, rank, me_ref, g_near_ref, g_far_ref, near_ref, far_ref, *refs):
    near_field_ref, far_field_ref, below_ref = refs[-3:]
    out_ref, own_ref = refs[-5:-3]
    step = pl.program_id(0)

    @pl.when(step == 0)
    def _():
        for half, field_ref in ((near_ref, near_field_ref), (far_ref, far_field_ref)):
            for z in range(half.shape[0]):
                field_ref[z * rows : (z + 1) * rows] = half[z, :rows, :width]

    product = jnp.dot(g_near_ref[...], near_field_ref[...], preferred_element_type=F32)
    product += jnp.dot(g_far_ref[...], far_field_ref[...], preferred_element_type=F32)
    per_step = out_ref.shape[0]
    for k in range(per_step):
        block = product[k * rows : (k + 1) * rows]
        out_ref[k, :rows] = block.astype(BF16)

        @pl.when(me_ref[0] == step * per_step + k)
        def _():
            own_ref[...] = block

    if share:

        @pl.when(step == 0)
        def _():
            t_ref, near_k_ref, far_k_ref, near_first_ref, far_first_ref = refs[:5]
            depth = near_ref.shape[0] * rows
            images = [
                half[:, :rows, half.shape[2] - rank :].reshape(depth, rank)
                for half in (near_k_ref, far_k_ref)
            ]
            firsts = [
                half[:, :rows, :width].reshape(depth, width)
                for half in (near_first_ref, far_first_ref)
            ]
            values = [t_ref[...]]
            for others in (firsts, (near_field_ref[...], far_field_ref[...])):
                total = sum(
                    lax.dot_general(
                        image, other, (((0,), (0,)), ((), ())), preferred_element_type=F32
                    )
                    for image, other in zip(images, others)
                )
                mine = jnp.zeros((share, width), F32)
                for i in range(rank // share):
                    mine = jnp.where(me_ref[1] == i, total[i * share : (i + 1) * share], mine)
                values.append(mine)
            below_ref[...] = jnp.concatenate(in_two(jnp.concatenate(values, axis=0)), axis=0)

        for k in range(per_step):
            out_ref[k, rows:] = below_ref[...]
    elif out_ref.shape[1] > rows:
        for k in range(per_step):
            out_ref[k, rows:] = refs[0][k]


def in_two(values):
    top = values.astype(BF16)
    return top, (values - top.astype(F32)).astype(BF16)


def send_coefficients(field, basis_ref, sent_refs):
    top, rest = in_two(field)
    terms = jnp.concatenate([top, rest, top], axis=0)
    coefficients = jnp.dot(basis_ref[...], terms, preferred_element_type=F32).astype(BF16)
    rank = sent_refs[0].shape[0]
    for bit, ref in enumerate(sent_refs):
        ref[...] = coefficients[bit * rank : (bit + 1) * rank]


def coefficients_kernel(field_ref, basis_ref, *sent_refs):
    send_coefficients(field_ref[...], basis_ref, sent_refs)


def image_kernel(me_ref, variance_ref, arrived_ref, own_ref, field_ref, *refs):
    rows = own_ref.shape[0]

    def add(d, total):
        part = arrived_ref[d, :rows].astype(F32)
        return total + jnp.where(me_ref[0] == d, jnp.zeros_like(part), part)

    total = lax.fori_loop(0, arrived_ref.shape[0], add, own_ref[...])
    image = variance_ref[0] * total + variance_ref[1] * field_ref[...]
    if len(refs) == 1:
        refs[0][...] = image
    else:
        refs[1][...] = image
        send_coefficients(image, refs[0], refs[2:])


def lift_kernel(levels, cuts, inside, field_ref, own_ref, lift_ref, *refs):
    outs = refs[-2 * len(cuts) :]
    arrived, extra = refs[:levels], refs[levels : -2 * len(cuts)]
    rank = arrived[0].shape[0]
    rows = field_ref.shape[0]
    terms = sum(
        jnp.dot(
            lift_ref[:, bit * rank : (bit + 1) * rank],
            arrived[bit][...],
            preferred_element_type=F32,
        )
        for bit in range(levels)
    )
    field = jnp.dot(own_ref[...], field_ref[...], precision=EXACT, preferred_element_type=F32)
    field = field + (terms[:rows] + terms[rows:])
    beside = [ref for ref in extra if ref.shape[0] == rows]
    below = [ref for ref in extra if ref.shape[0] != rows]
    for k, (start, stop) in enumerate(cuts):
        out_ref, sent_ref = outs[2 * k : 2 * k + 2]
        part = field[:, start:stop]
        whole = part
        if beside and k == 0:
            whole = jnp.concatenate([part, beside[0][...]], axis=1)
        out_ref[...] = whole if inside else part
        whole = whole.astype(BF16)
        for copy in range(sent_ref.shape[0]):
            sent_ref[copy, :rows] = whole
            for ref in below:
                sent_ref[copy, rows:] = ref[...]


def kernel_call(kernel, shapes, operands, scalars=0, scratch=()):
    in_smem = [pl.BlockSpec(memory_space=pltpu.SMEM)] * scalars
    in_vmem = [pl.BlockSpec(memory_space=pltpu.VMEM)] * (len(operands) - scalars)
    return pl.pallas_call(
        kernel,
        out_shape=[jax.ShapeDtypeStruct(shape, dtype) for shape, dtype in shapes],
        in_specs=in_smem + in_vmem,
        out_specs=[pl.BlockSpec(memory_space=pltpu.VMEM)] * len(shapes),
        scratch_shapes=[pltpu.VMEM(shape, dtype) for shape, dtype in scratch],
        interpret=INTERPRET,
    )(*operands)


def local(grm, right_sides, inv_diag, bases, couplings, level_map, variance, iters_per_column):
    rows, rhs = right_sides.shape
    levels = couplings.shape[0] - 1
    rank = couplings.shape[1]
    split_at = levels * rank
    n_rows, n_columns = lax.axis_size(ROWS), lax.axis_size(COLUMNS)
    me_rows, me_columns = lax.axis_index(ROWS), lax.axis_index(COLUMNS)

    old = lax.broadcasted_iota(jnp.int32, (split_at, split_at), 0)
    new = jnp.repeat(level_map, rank) * rank + jnp.arange(split_at, dtype=jnp.int32) % rank
    shuffle = (old == new[None, :]).astype(F32)
    by_bit = mm3(bases[:, :split_at], shuffle)
    coarse_basis = bases[:, split_at:]

    scale = 1.0 / (n_rows * n_columns * jnp.max(jnp.abs(couplings)))
    couplings = couplings * scale
    diag = (inv_diag * scale)[:, None]
    coarse_coupling = couplings[levels]
    column = lax.broadcasted_iota(jnp.int32, (split_at, split_at), 1)
    repeat = (
        lax.broadcasted_iota(jnp.int32, (rank, split_at), 0)
        == lax.broadcasted_iota(jnp.int32, (rank, split_at), 1) % rank
    )
    tiled = mm3(couplings[:levels].reshape(split_at, rank), repeat.astype(F32))
    old_rows = lax.broadcasted_iota(jnp.int32, (split_at, split_at), 0)
    diagonal_blocks = jnp.where(old_rows // rank == column // rank, tiled, 0.0)
    lift = mm3(mm3(bases[:, :split_at], diagonal_blocks), shuffle)
    lift_terms = two_terms(lift)
    eye = lax.broadcasted_iota(jnp.int32, (rows, rows), 0) == jnp.arange(rows)[None]
    own_lift = mm3(lift, by_bit.T) + jnp.where(eye, diag, 0.0)
    basis_top, basis_rest = jnp.split(two_terms(by_bit.T), 2, axis=0)
    basis_terms = jnp.concatenate([basis_top, basis_top, basis_rest], axis=1)

    def coefficient_shapes(columns):
        return [((rank, columns), BF16)] * levels

    def precondition(field, sent, cuts=None, inside=False, beside=None, below=None):
        far = [("x", 1), ("x", 2), ("z", 1), ("z", 2), ("z", 4), ("c", 1), ("y", 1), ("y", 2)]
        order = [5, 0, 6, 2, 1, 7, 3, 4]
        arrived = {bit: from_partner(sent[bit], *far[bit]) for bit in order}
        extra = [array for array in (beside, below) if array is not None]
        more_rows = 0 if below is None else below.shape[0]
        cuts = cuts or [(0, field.shape[1])]
        shapes = []
        for k, (start, stop) in enumerate(cuts):
            more = beside.shape[1] if beside is not None and k == 0 else 0
            shapes.append(((rows, stop - start + (more if inside else 0)), F32))
            copies = (lax.axis_size("z"), rows + more_rows, stop - start + more)
            shapes.append((copies, BF16))
        return kernel_call(
            functools.partial(lift_kernel, levels, cuts, inside),
            shapes,
            [field, own_lift, lift_terms, *[arrived[bit] for bit in range(levels)], *extra],
        )

    places = jnp.stack([me_rows, me_columns]).astype(jnp.int32)
    right_sides, *blocks = lax.optimization_barrier((right_sides, *cut_by_x(grm)))
    sent = kernel_call(coefficients_kernel, coefficient_shapes(rhs), [right_sides, basis_terms])
    g_blocks = rearranged(blocks)

    def gathered(copies):
        near = exchanged(copies, "z")
        return near, shifted(near, "c", 1)

    def products(everyone, width, riders=(), more_rows=0, share=0):
        depth = lax.axis_size("z") * rows
        per_step = n_rows // 4
        height = rows + more_rows

        def whole(array):
            return pl.BlockSpec(array.shape, lambda i: (0,) * array.ndim)

        def some(shape):
            return pl.BlockSpec(shape, lambda i: (i,) + (0,) * (len(shape) - 1))

        rider_specs = [whole(array) for array in riders]
        if riders and not share:
            rider_specs = [some((per_step, *riders[0].shape[1:]))]
        partial, own = pl.pallas_call(
            functools.partial(times_kernel, rows, width, share, rank),
            grid=(4,),
            out_shape=[
                jax.ShapeDtypeStruct((n_rows, height, width), BF16),
                jax.ShapeDtypeStruct((rows, width), F32),
            ],
            in_specs=[
                pl.BlockSpec(memory_space=pltpu.SMEM),
                *[some((per_step * rows, depth))] * 2,
                *[whole(array) for array in everyone],
                *rider_specs,
            ],
            out_specs=[some((per_step, height, width)), pl.BlockSpec((rows, width), lambda i: (0, 0))],
            scratch_shapes=[
                *[pltpu.VMEM((depth, width), BF16)] * 2,
                pltpu.VMEM((more_rows or 8, width), BF16),
            ],
            name="times",
            interpret=INTERPRET,
        )(places, *g_blocks, *everyone, *riders)
        return exchanged(partial, ROWS), own

    def image_of(arrived, own, field, send=True):
        width = field.shape[1]
        shapes = [((rows, width), F32)] + (coefficient_shapes(width) if send else [])
        operands = [places, variance, arrived, own, field] + ([basis_terms] if send else [])
        image, *sent = kernel_call(image_kernel, shapes, operands, 2)
        return image, sent

    def sum_of_terms(terms, axis):
        top, rest = jnp.split(terms.astype(F32), 2, axis=axis)
        return top + rest

    half = rhs // PARTS
    cuts = [(k * half, (k + 1) * half) for k in range(PARTS)]
    widths = [half + (0 if k else rank) for k in range(PARTS)]
    parts = range(len(cuts))

    def padded(array, width):
        more = width - array.shape[-1]
        return jnp.pad(array, [(0, 0)] * (array.ndim - 1) + [(0, more)])

    share = rank // n_columns
    t_share = rank // n_rows
    t_parts = mm3(coarse_basis.T, right_sides).reshape(n_rows, t_share, rhs)
    t_top = lax.reduce_precision(t_parts, 8, 7)
    t_parts = jnp.concatenate([t_top, t_parts - t_top], axis=1).astype(BF16)
    t_parts = [padded(t_parts[:, :, slice(*cuts[k])], widths[k]) for k in parts]

    first = precondition(right_sides, sent, cuts, True, beside=coarse_basis)
    first, copies = first[::2], first[1::2]
    all_first = [gathered(copies[k]) for k in parts]
    sums = [products(all_first[k], widths[k], [t_parts[k]], 2 * t_share) for k in parts]
    first_image, sent = zip(*[image_of(*sums[k], first[k]) for k in parts])
    coarse_image = first_image[0][:, half:]

    second, all_second, t_rows = [], [], []
    for k in parts:
        rows_of_t = sum_of_terms(sums[k][0][:, rows:], 1).sum(axis=0)
        field, copies = precondition(
            first_image[k],
            sent[k],
            beside=None if k else coarse_image,
            below=two_terms(padded(rows_of_t, widths[k] + (0 if k else rank))),
        )
        second.append(field)
        all_second.append(gathered(copies))
        near, far = all_second[k]
        rode = near[:, rows:, : widths[k]].astype(F32) + far[:, rows:, : widths[k]].astype(F32)
        t_rows.append(sum_of_terms(rode, 1).sum(axis=0))
    sums = [
        products(
            all_second[k], widths[k], [t_rows[k], *all_second[0], *all_first[k]], 6 * share, share
        )
        for k in parts
    ]
    second_image, sent = zip(*[image_of(*sums[k], second[k]) for k in parts])

    t0, third, third_image, tables = [], [], [], []
    for k in parts:
        rode = sum_of_terms(sums[k][0][:, rows:], 1)
        t0.append(rode[:, :t_share].reshape(rank, widths[k])[:, :half])
        field, copies = precondition(
            second_image[k], sent[k], below=two_terms(rode[:, t_share:].sum(axis=0))
        )
        third.append(field)
        everyone = gathered(copies)
        arrived, own = products(everyone, widths[k])
        own, *everyone = lax.optimization_barrier((own, *everyone))
        third_image.append(image_of(arrived, own, field, send=False)[0])
        table = sum_of_terms(jnp.stack([array[:, rows:] for array in everyone]), 2)
        table = jnp.where(lax.axis_index("c") == 0, table, table[::-1])
        table = table.reshape(n_columns, 2, share, widths[k]).transpose(1, 0, 2, 3)
        tables.append(table.reshape(2, rank, widths[k]))

    def joined(fields):
        if PARTS == 1:
            return fields[0]
        return jnp.concatenate([fields[0][:, :half], *fields[1:], fields[0][:, half:]], axis=1)

    first, second, third = joined(first), joined(second), joined(third)
    first_image, second_image = joined(first_image), joined(second_image)
    third_image = joined(third_image)
    t0 = jnp.concatenate(t0, axis=1)
    k_first, k_second = (joined([table[i] for table in tables]) for i in range(2))

    k_basis = k_first[:, rhs:]
    s0 = mm(coarse_coupling, t0[:, :rhs])
    s1 = mm(coarse_coupling, k_first[:, :rhs] + mm(k_basis, s0))
    s2 = mm(coarse_coupling, k_second[:, :rhs] + mm(k_second[:, rhs:], s0) + mm(k_basis, s1))
    weights = jnp.concatenate([s0, s1, s2], axis=0)

    none = jnp.zeros_like(coarse_basis)
    coarse_parts = jnp.concatenate(
        [
            jnp.concatenate([coarse_basis, none, none], axis=1),
            jnp.concatenate([second[:, rhs:], coarse_basis, none], axis=1),
            jnp.concatenate([third[:, rhs:], second[:, rhs:], coarse_basis], axis=1),
            jnp.concatenate([coarse_image, none, none], axis=1),
            jnp.concatenate([second_image[:, rhs:], coarse_image, none], axis=1),
        ],
        axis=0,
    )
    coarse_parts = mm3(coarse_parts, weights).reshape(5, rows, rhs)
    v = [field[:, :rhs] + coarse_parts[k] for k, field in enumerate([first, second, third])]
    w = [right_sides]
    w += [field[:, :rhs] + coarse_parts[3 + k] for k, field in enumerate([first_image, second_image])]
    last_parts = [third_image[:, rhs:], second_image[:, rhs:], coarse_image]
    w.append(third_image[:, :rhs] + mm3(jnp.concatenate(last_parts, axis=1), weights))

    moments = jnp.stack([jnp.sum(w[k - k // 2] * v[k // 2], axis=0) for k in range(2 * STEPS)])
    moments = from_everyone(moments, ROWS).sum(axis=0)
    moments = from_everyone(moments, COLUMNS).sum(axis=0)

    m = [moments[k] for k in range(2 * STEPS)]
    one, zero = jnp.ones_like(m[0]), jnp.zeros_like(m[0])
    in_r, kept_r, kept_x, direction, energy = [one], [one], [], [], None
    for step in range(STEPS):
        basis = range(step + 1)
        fresh = sum(in_r[p] * in_r[q] * m[p + q] for p in basis for q in basis)
        before = [fresh / energy * d for d in direction] if step else []
        direction = [r + d for r, d in zip(in_r, before + [zero])]
        energy = fresh
        alpha = energy / sum(direction[p] * direction[q] * m[p + q + 1] for p in basis for q in basis)
        in_r = [a - b for a, b in zip(in_r + [zero], [zero] + [alpha * d for d in direction])]
        active = step < iters_per_column
        kept_r = [jnp.where(active, a, b) for a, b in zip(in_r, kept_r + [zero])]
        kept_x = [jnp.where(active, b + alpha * d, b) for d, b in zip(direction, kept_x + [zero])]

    solution = sum(c * field for c, field in zip(kept_x, v))
    residual = w[0] + sum(c * field for c, field in zip(kept_r[1:], w[1:]))
    return (solution, residual)


def solution(mesh):
    split = Mesh(mesh.devices.reshape(4, 2, 8, 4), HI_LO)
    return jax.shard_map(
        local,
        mesh=split,
        in_specs=(
            P(None, LO, None, HI, None),
            P(HI_LO, None),
            P(HI_LO),
            P(HI_LO, None),
            P(),
            P(),
            P(),
            P(),
        ),
        out_specs=(P(HI_LO, None), P(HI_LO, None)),
        check_vma=False,
    )
```

```python
import functools

import jax
import jax.numpy as jnp
from jax import lax
from jax.experimental import pallas as pl
from jax.experimental.pallas import tpu as pltpu
from jax.sharding import Mesh
from jax.sharding import PartitionSpec as P


HI = ("y", "c")
LO = ("z", "x")
HI_LO = ("y", "c", "z", "x")
COLUMNS = ("c", "z")
ROWS = ("y", "x")
BF16 = jnp.bfloat16
F32 = jnp.float32
EXACT = lax.Precision.HIGHEST
STEPS = 3
INTERPRET = False


def mm(left, right):
    return jnp.dot(left, right, precision=EXACT)


def mm3(left, right):
    return jnp.dot(left, right, precision=lax.Precision.HIGH)


def from_everyone(array, axes):
    copies = jnp.broadcast_to(array, (lax.axis_size(axes), *array.shape))
    return lax.all_to_all(copies, axes, split_axis=0, concat_axis=0, tiled=True)


def exchanged(array, axes):
    return lax.all_to_all(array, axes, split_axis=0, concat_axis=0, tiled=True)


def shifted(value, axis, step):
    size = lax.axis_size(axis)
    return lax.ppermute(value, axis, [(i, (i + step) % size) for i in range(size)])


def from_partner(value, axis, distance):
    return lax.ppermute(value, axis, [(i, i ^ distance) for i in range(lax.axis_size(axis))])


def two_terms(values):
    top = lax.reduce_precision(values, 8, 7)
    return jnp.concatenate([top, values - top], axis=0).astype(BF16)


def by_x_kernel(n_x, n_z, me_ref, grm_ref, *out_refs):
    rows = grm_ref.shape[1]

    def regroup(block, _):
        whole = grm_ref[block]
        columns = []
        for x in range(n_x):
            starts = [(z * n_x + x) * rows for z in range(n_z)]
            columns.append(jnp.concatenate([whole[:, at : at + rows] for at in starts], axis=1))
        for step, out_ref in enumerate(out_refs):
            wanted = lax.rem(me_ref[0] + step, n_x)
            chosen = columns[0]
            for x in range(1, n_x):
                chosen = jnp.where(wanted == x, columns[x], chosen)
            out_ref[block] = chosen
        return 0

    lax.fori_loop(0, grm_ref.shape[0], regroup, 0)


def place_kernel(n_x, n_c, me_ref, *refs):
    arrived, (kept_ref, other_ref) = refs[:n_x], refs[n_x:]
    for step, ref in enumerate(arrived):
        x = lax.rem(me_ref[0] - step + n_x, n_x)
        for y in range(ref.shape[0] // n_c):
            kept_ref[y, x] = ref[y * n_c + me_ref[1]]
            other_ref[y, x] = ref[y * n_c + 1 - me_ref[1]]


def cut_by_x(grm):
    n_y, n_c, n_z, n_x = (lax.axis_size(name) for name in HI_LO)
    rows = grm.shape[2]
    me = lax.axis_index("x").astype(jnp.int32)[None]
    depth = n_z * rows
    return kernel_call(
        functools.partial(by_x_kernel, n_x, n_z),
        [((n_y * n_c, rows, depth), grm.dtype)] * n_x,
        [me, grm.reshape(n_y * n_c, rows, n_x * depth)],
        1,
    )


def rearranged(blocks):
    n_y, n_c, _, n_x = (lax.axis_size(name) for name in HI_LO)
    _, rows, depth = blocks[0].shape
    me = jnp.stack([lax.axis_index("x"), lax.axis_index("c")]).astype(jnp.int32)
    arrived = [shifted(block, "x", k) if k else block for k, block in enumerate(blocks)]
    kept, other = kernel_call(
        functools.partial(place_kernel, n_x, n_c),
        [((n_y, n_x, rows, depth), BF16)] * 2,
        [me, *arrived],
        1,
    )
    return kept.reshape(-1, depth), shifted(other, "c", 1).reshape(-1, depth)


def times_kernel(rows, width, share, rank, me_ref, g_near_ref, g_far_ref, near_ref, far_ref, *refs):
    near_field_ref, far_field_ref, below_ref = refs[-3:]
    out_ref, own_ref = refs[-5:-3]
    step = pl.program_id(0)

    @pl.when(step == 0)
    def _():
        for half, field_ref in ((near_ref, near_field_ref), (far_ref, far_field_ref)):
            for z in range(half.shape[0]):
                field_ref[z * rows : (z + 1) * rows] = half[z, :rows, :width]

    product = jnp.dot(g_near_ref[...], near_field_ref[...], preferred_element_type=F32)
    product += jnp.dot(g_far_ref[...], far_field_ref[...], preferred_element_type=F32)
    per_step = out_ref.shape[0]
    for k in range(per_step):
        block = product[k * rows : (k + 1) * rows]
        out_ref[k, :rows] = block.astype(BF16)

        @pl.when(me_ref[0] == step * per_step + k)
        def _():
            own_ref[...] = block

    if share:

        @pl.when(step == 0)
        def _():
            t_ref, near_k_ref, far_k_ref, near_first_ref, far_first_ref = refs[:5]
            depth = near_ref.shape[0] * rows
            images = [
                half[:, :rows, half.shape[2] - rank :].reshape(depth, rank)
                for half in (near_k_ref, far_k_ref)
            ]
            firsts = [
                half[:, :rows, :width].reshape(depth, width)
                for half in (near_first_ref, far_first_ref)
            ]
            values = [t_ref[...]]
            for others in (firsts, (near_field_ref[...], far_field_ref[...])):
                total = sum(
                    lax.dot_general(
                        image, other, (((0,), (0,)), ((), ())), preferred_element_type=F32
                    )
                    for image, other in zip(images, others)
                )
                mine = jnp.zeros((share, width), F32)
                for i in range(rank // share):
                    mine = jnp.where(me_ref[1] == i, total[i * share : (i + 1) * share], mine)
                values.append(mine)
            below_ref[...] = jnp.concatenate(in_two(jnp.concatenate(values, axis=0)), axis=0)

        for k in range(per_step):
            out_ref[k, rows:] = below_ref[...]
    elif out_ref.shape[1] > rows:
        for k in range(per_step):
            out_ref[k, rows:] = refs[0][k]


def in_two(values):
    top = values.astype(BF16)
    return top, (values - top.astype(F32)).astype(BF16)


def send_coefficients(field, basis_ref, sent_refs):
    top, rest = in_two(field)
    terms = jnp.concatenate([top, rest, top], axis=0)
    coefficients = jnp.dot(basis_ref[...], terms, preferred_element_type=F32).astype(BF16)
    rank = sent_refs[0].shape[0]
    for bit, ref in enumerate(sent_refs):
        ref[...] = coefficients[bit * rank : (bit + 1) * rank]


def coefficients_kernel(field_ref, basis_ref, *sent_refs):
    send_coefficients(field_ref[...], basis_ref, sent_refs)


def image_kernel(with_coarse, me_ref, variance_ref, arrived_ref, own_ref, field_ref, *refs):
    rows = own_ref.shape[0]

    def add(d, total):
        part = arrived_ref[d, :rows].astype(F32)
        return total + jnp.where(me_ref[0] == d, jnp.zeros_like(part), part)

    total = lax.fori_loop(0, arrived_ref.shape[0], add, own_ref[...])
    image = variance_ref[0] * total + variance_ref[1] * field_ref[...]
    if len(refs) == 1:
        refs[0][...] = image
        return
    if not with_coarse:
        refs[1][...] = image
        send_coefficients(image, refs[0], refs[2:])
        return
    basis_ref, coupling_ref, image_ref, coarse_ref, s0_ref = refs[:5]
    rank = coupling_ref.shape[0]
    rhs = image.shape[1] - rank
    share = (arrived_ref.shape[1] - rows) // 6
    pieces = []
    for d in range(arrived_ref.shape[0]):
        rode = arrived_ref[d, rows:, :rhs].astype(F32)
        pieces.append(rode[:share] + rode[3 * share : 4 * share])
    t0 = jnp.concatenate(pieces, axis=0)
    s0 = jnp.dot(coupling_ref[...], t0, precision=EXACT, preferred_element_type=F32)
    coarse = image[:, rhs:]
    image = image[:, :rhs] + jnp.dot(coarse, s0, precision=EXACT, preferred_element_type=F32)
    image_ref[...] = image
    coarse_ref[...] = coarse
    s0_ref[...] = s0
    send_coefficients(image, basis_ref, refs[5:])


def lift_kernel(levels, cuts, inside, field_ref, own_ref, lift_ref, *refs):
    outs = refs[-2 * len(cuts) :]
    arrived, extra = refs[:levels], refs[levels : -2 * len(cuts)]
    rank = arrived[0].shape[0]
    rows = field_ref.shape[0]
    terms = sum(
        jnp.dot(
            lift_ref[:, bit * rank : (bit + 1) * rank],
            arrived[bit][...],
            preferred_element_type=F32,
        )
        for bit in range(levels)
    )
    field = jnp.dot(own_ref[...], field_ref[...], precision=EXACT, preferred_element_type=F32)
    field = field + (terms[:rows] + terms[rows:])
    beside = [ref for ref in extra if ref.shape[0] == rows]
    below = [ref for ref in extra if ref.shape[0] != rows]
    for k, (start, stop) in enumerate(cuts):
        out_ref, sent_ref = outs[2 * k : 2 * k + 2]
        part = field[:, start:stop]
        whole = part
        if beside and k == 0:
            whole = jnp.concatenate([part, beside[0][...]], axis=1)
        out_ref[...] = whole if inside else part
        whole = whole.astype(BF16)
        for copy in range(sent_ref.shape[0]):
            sent_ref[copy, :rows] = whole
            for ref in below:
                sent_ref[copy, rows:] = ref[...]


def kernel_call(kernel, shapes, operands, scalars=0, scratch=()):
    in_smem = [pl.BlockSpec(memory_space=pltpu.SMEM)] * scalars
    in_vmem = [pl.BlockSpec(memory_space=pltpu.VMEM)] * (len(operands) - scalars)
    return pl.pallas_call(
        kernel,
        out_shape=[jax.ShapeDtypeStruct(shape, dtype) for shape, dtype in shapes],
        in_specs=in_smem + in_vmem,
        out_specs=[pl.BlockSpec(memory_space=pltpu.VMEM)] * len(shapes),
        scratch_shapes=[pltpu.VMEM(shape, dtype) for shape, dtype in scratch],
        interpret=INTERPRET,
    )(*operands)


def local(grm, right_sides, inv_diag, bases, couplings, level_map, variance, iters_per_column):
    rows, rhs = right_sides.shape
    levels = couplings.shape[0] - 1
    rank = couplings.shape[1]
    split_at = levels * rank
    width = rhs + rank
    n_rows, n_columns = lax.axis_size(ROWS), lax.axis_size(COLUMNS)
    me_rows, me_columns = lax.axis_index(ROWS), lax.axis_index(COLUMNS)

    old = lax.broadcasted_iota(jnp.int32, (split_at, split_at), 0)
    new = jnp.repeat(level_map, rank) * rank + jnp.arange(split_at, dtype=jnp.int32) % rank
    shuffle = (old == new[None, :]).astype(F32)
    by_bit = mm3(bases[:, :split_at], shuffle)
    coarse_basis = bases[:, split_at:]

    scale = 1.0 / (n_rows * n_columns * jnp.max(jnp.abs(couplings)))
    couplings = couplings * scale
    diag = (inv_diag * scale)[:, None]
    coarse_coupling = couplings[levels]
    column = lax.broadcasted_iota(jnp.int32, (split_at, split_at), 1)
    repeat = (
        lax.broadcasted_iota(jnp.int32, (rank, split_at), 0)
        == lax.broadcasted_iota(jnp.int32, (rank, split_at), 1) % rank
    )
    tiled = mm3(couplings[:levels].reshape(split_at, rank), repeat.astype(F32))
    old_rows = lax.broadcasted_iota(jnp.int32, (split_at, split_at), 0)
    diagonal_blocks = jnp.where(old_rows // rank == column // rank, tiled, 0.0)
    lift = mm3(mm3(bases[:, :split_at], diagonal_blocks), shuffle)
    lift_terms = two_terms(lift)
    eye = lax.broadcasted_iota(jnp.int32, (rows, rows), 0) == jnp.arange(rows)[None]
    own_lift = mm3(lift, by_bit.T) + jnp.where(eye, diag, 0.0)
    basis_top, basis_rest = jnp.split(two_terms(by_bit.T), 2, axis=0)
    basis_terms = jnp.concatenate([basis_top, basis_top, basis_rest], axis=1)

    def coefficient_shapes(columns):
        return [((rank, columns), BF16)] * levels

    def precondition(field, sent, cuts=None, inside=False, beside=None, below=None):
        far = [("x", 1), ("x", 2), ("z", 1), ("z", 2), ("z", 4), ("c", 1), ("y", 1), ("y", 2)]
        order = [5, 0, 6, 2, 1, 7, 3, 4]
        arrived = {bit: from_partner(sent[bit], *far[bit]) for bit in order}
        extra = [array for array in (beside, below) if array is not None]
        more_rows = 0 if below is None else below.shape[0]
        cuts = cuts or [(0, field.shape[1])]
        shapes = []
        for k, (start, stop) in enumerate(cuts):
            more = beside.shape[1] if beside is not None and k == 0 else 0
            shapes.append(((rows, stop - start + (more if inside else 0)), F32))
            copies = (lax.axis_size("z"), rows + more_rows, stop - start + more)
            shapes.append((copies, BF16))
        return kernel_call(
            functools.partial(lift_kernel, levels, cuts, inside),
            shapes,
            [field, own_lift, lift_terms, *[arrived[bit] for bit in range(levels)], *extra],
        )

    places = jnp.stack([me_rows, me_columns]).astype(jnp.int32)
    right_sides, *blocks = lax.optimization_barrier((right_sides, *cut_by_x(grm)))
    sent = kernel_call(coefficients_kernel, coefficient_shapes(rhs), [right_sides, basis_terms])
    g_blocks = rearranged(blocks)

    def gathered(copies):
        near = exchanged(copies, "z")
        return near, shifted(near, "c", 1)

    def products(everyone, width, riders=(), more_rows=0, share=0):
        depth = lax.axis_size("z") * rows
        per_step = n_rows // 4
        height = rows + more_rows

        def whole(array):
            return pl.BlockSpec(array.shape, lambda i: (0,) * array.ndim)

        def some(shape):
            return pl.BlockSpec(shape, lambda i: (i,) + (0,) * (len(shape) - 1))

        rider_specs = [whole(array) for array in riders]
        if riders and not share:
            rider_specs = [some((per_step, *riders[0].shape[1:]))]
        partial, own = pl.pallas_call(
            functools.partial(times_kernel, rows, width, share, rank),
            grid=(4,),
            out_shape=[
                jax.ShapeDtypeStruct((n_rows, height, width), BF16),
                jax.ShapeDtypeStruct((rows, width), F32),
            ],
            in_specs=[
                pl.BlockSpec(memory_space=pltpu.SMEM),
                *[some((per_step * rows, depth))] * 2,
                *[whole(array) for array in everyone],
                *rider_specs,
            ],
            out_specs=[some((per_step, height, width)), pl.BlockSpec((rows, width), lambda i: (0, 0))],
            scratch_shapes=[
                *[pltpu.VMEM((depth, width), BF16)] * 2,
                pltpu.VMEM((more_rows or 8, width), BF16),
            ],
            name="times",
            interpret=INTERPRET,
        )(places, *g_blocks, *everyone, *riders)
        return exchanged(partial, ROWS), own

    def image_of(arrived, own, field):
        width = field.shape[1]
        operands = [places, variance, arrived, own, field, basis_terms]
        shapes = [((rows, width), F32)] + coefficient_shapes(width)
        kernel = functools.partial(image_kernel, False)
        image, *sent = kernel_call(kernel, shapes, operands, 2)
        return image, sent

    def last_image_of(arrived, own, field):
        operands = [places, variance, arrived, own, field]
        kernel = functools.partial(image_kernel, False)
        return kernel_call(kernel, [(field.shape, F32)], operands, 2)[0]

    def image_with_coarse(arrived, own, field):
        operands = [places, variance, arrived, own, field, basis_terms, coarse_coupling]
        shapes = [((rows, rhs), F32), ((rows, rank), F32), ((rank, rhs), F32)]
        kernel = functools.partial(image_kernel, True)
        shapes = shapes + coefficient_shapes(rhs)
        image, coarse, s0, *sent = kernel_call(kernel, shapes, operands, 2)
        return image, coarse, s0, sent

    def sum_of_terms(terms, axis):
        top, rest = jnp.split(terms.astype(F32), 2, axis=axis)
        return top + rest

    def padded(array, width):
        more = width - array.shape[-1]
        return jnp.pad(array, [(0, 0)] * (array.ndim - 1) + [(0, more)])

    share = rank // n_columns
    t_share = rank // n_rows
    t_parts = mm3(coarse_basis.T, right_sides).reshape(n_rows, t_share, rhs)
    t_top = lax.reduce_precision(t_parts, 8, 7)
    t_parts = jnp.concatenate([t_top, t_parts - t_top], axis=1).astype(BF16)
    t_parts = padded(t_parts, width)

    cuts = [(0, rhs)]
    first, copies = precondition(right_sides, sent, cuts, True, beside=coarse_basis)
    all_first = gathered(copies)
    arrived, own = products(all_first, width, [t_parts], 2 * t_share)
    first_image, sent = image_of(arrived, own, first)
    coarse_image = first_image[:, rhs:]

    t_rows = sum_of_terms(arrived[:, rows:], 1).sum(axis=0)
    t_rows = two_terms(padded(t_rows, width + rank))
    second, copies = precondition(first_image, sent, beside=coarse_image, below=t_rows)
    all_second = gathered(copies)
    near, far = all_second
    t_rows = near[:, rows:, :width].astype(F32) + far[:, rows:, :width].astype(F32)
    t_rows = sum_of_terms(t_rows, 1).sum(axis=0)
    riders = [t_rows, *all_second, *all_first]
    arrived, own = products(all_second, width, riders, 6 * share, share)
    second_image, second_coarse, s0, sent = image_with_coarse(arrived, own, second)

    rode = sum_of_terms(arrived[:, rows:], 1)[:, t_share:].sum(axis=0)
    below = [rode[:, :rhs], rode[:, rhs:].reshape(-1, rhs)]
    below = two_terms(jnp.concatenate(below, axis=0))
    n_below = below.shape[0]
    below = jnp.pad(below, ((0, -n_below % 8), (0, 0)))
    third, copies = precondition(second_image, sent, below=below)
    everyone = gathered(copies)
    arrived, own = products(everyone, rhs)
    own, *everyone = lax.optimization_barrier((own, *everyone))
    third_image = last_image_of(arrived, own, third)

    table = sum_of_terms(jnp.stack([array[:, rows : rows + n_below] for array in everyone]), 2)
    table = jnp.where(lax.axis_index("c") == 0, table, table[::-1])
    table = table.reshape(n_columns, n_below // 2, rhs)
    k_first = table[:, :share].reshape(rank, rhs)
    k_second = table[:, share : 2 * share].reshape(rank, rhs)
    k_coarse = table[:, 2 * share :].reshape(n_columns, 2, share, rank).transpose(1, 0, 2, 3)
    k_basis, k_coarse = k_coarse.reshape(2, rank, rank)
    s1 = mm(coarse_coupling, k_first + mm(k_basis, s0))
    s2 = mm(coarse_coupling, k_second + mm(k_coarse, s0) + mm(k_basis, s1))
    weights = jnp.concatenate([s0, s1, s2], axis=0)

    none = jnp.zeros_like(coarse_basis)
    second_lift = second[:, rhs:]
    coarse_parts = [
        [coarse_basis, none, none],
        [second_lift, coarse_basis, none],
        [none, second_lift, coarse_basis],
        [coarse_image, none, none],
        [none, coarse_image, none],
        [none, second_coarse, coarse_image],
    ]
    coarse_parts = jnp.concatenate([jnp.concatenate(row, axis=1) for row in coarse_parts], axis=0)
    coarse_parts = mm3(coarse_parts, weights).reshape(6, rows, rhs)
    fields = [first[:, :rhs], second[:, :rhs], third]
    v = [field + part for field, part in zip(fields, coarse_parts[:3])]
    fields = [first_image[:, :rhs], second_image, third_image]
    w = [right_sides] + [field + part for field, part in zip(fields, coarse_parts[3:])]

    moments = jnp.stack([jnp.sum(w[k - k // 2] * v[k // 2], axis=0) for k in range(2 * STEPS)])
    moments = from_everyone(moments, ROWS).sum(axis=0)
    moments = from_everyone(moments, COLUMNS).sum(axis=0)

    m = [moments[k] for k in range(2 * STEPS)]
    one, zero = jnp.ones_like(m[0]), jnp.zeros_like(m[0])
    in_r, kept_r, kept_x, direction, energy = [one], [one], [], [], None
    for step in range(STEPS):
        basis = range(step + 1)
        fresh = sum(in_r[p] * in_r[q] * m[p + q] for p in basis for q in basis)
        before = [fresh / energy * d for d in direction] if step else []
        direction = [r + d for r, d in zip(in_r, before + [zero])]
        energy = fresh
        alpha = energy / sum(direction[p] * direction[q] * m[p + q + 1] for p in basis for q in basis)
        in_r = [a - b for a, b in zip(in_r + [zero], [zero] + [alpha * d for d in direction])]
        active = step < iters_per_column
        kept_r = [jnp.where(active, a, b) for a, b in zip(in_r, kept_r + [zero])]
        kept_x = [jnp.where(active, b + alpha * d, b) for d, b in zip(direction, kept_x + [zero])]

    solution = sum(c * field for c, field in zip(kept_x, v))
    residual = w[0] + sum(c * field for c, field in zip(kept_r[1:], w[1:]))
    return (solution, residual)


def solution(mesh):
    split = Mesh(mesh.devices.reshape(4, 2, 8, 4), HI_LO)
    return jax.shard_map(
        local,
        mesh=split,
        in_specs=(
            P(None, LO, None, HI, None),
            P(HI_LO, None),
            P(HI_LO),
            P(HI_LO, None),
            P(),
            P(),
            P(),
            P(),
        ),
        out_specs=(P(HI_LO, None), P(HI_LO, None)),
        check_vma=False,
    )
```

```python
import functools

import jax
import jax.numpy as jnp
from jax import lax
from jax.experimental import pallas as pl
from jax.experimental.pallas import tpu as pltpu
from jax.sharding import Mesh
from jax.sharding import PartitionSpec as P


HI = ("y", "c")
LO = ("z", "x")
HI_LO = ("y", "c", "z", "x")
COLUMNS = ("c", "z")
ROWS = ("y", "x")
BF16 = jnp.bfloat16
F32 = jnp.float32
EXACT = lax.Precision.HIGHEST
STEPS = 3
INTERPRET = False


def mm(left, right):
    return jnp.dot(left, right, precision=EXACT)


def mm3(left, right):
    return jnp.dot(left, right, precision=lax.Precision.HIGH)


def from_everyone(array, axes):
    copies = jnp.broadcast_to(array, (lax.axis_size(axes), *array.shape))
    return lax.all_to_all(copies, axes, split_axis=0, concat_axis=0, tiled=True)


def exchanged(array, axes):
    return lax.all_to_all(array, axes, split_axis=0, concat_axis=0, tiled=True)


def shifted(value, axis, step):
    size = lax.axis_size(axis)
    return lax.ppermute(value, axis, [(i, (i + step) % size) for i in range(size)])


def from_partner(value, axis, distance):
    return lax.ppermute(value, axis, [(i, i ^ distance) for i in range(lax.axis_size(axis))])


def two_terms(values):
    top = lax.reduce_precision(values, 8, 7)
    return jnp.concatenate([top, values - top], axis=0).astype(BF16)


def by_x_kernel(n_x, n_z, me_ref, grm_ref, *out_refs):
    rows = grm_ref.shape[1]

    def regroup(block, _):
        whole = grm_ref[block]
        columns = []
        for x in range(n_x):
            starts = [(z * n_x + x) * rows for z in range(n_z)]
            columns.append(jnp.concatenate([whole[:, at : at + rows] for at in starts], axis=1))
        for step, out_ref in enumerate(out_refs):
            wanted = lax.rem(me_ref[0] + step, n_x)
            chosen = columns[0]
            for x in range(1, n_x):
                chosen = jnp.where(wanted == x, columns[x], chosen)
            out_ref[block] = chosen
        return 0

    lax.fori_loop(0, grm_ref.shape[0], regroup, 0)


def place_kernel(n_x, n_c, me_ref, *refs):
    arrived, (kept_ref, other_ref) = refs[:n_x], refs[n_x:]
    for step, ref in enumerate(arrived):
        x = lax.rem(me_ref[0] - step + n_x, n_x)
        for y in range(ref.shape[0] // n_c):
            kept_ref[y, x] = ref[y * n_c + me_ref[1]]
            other_ref[y, x] = ref[y * n_c + 1 - me_ref[1]]


def cut_by_x(grm):
    n_y, n_c, n_z, n_x = (lax.axis_size(name) for name in HI_LO)
    rows = grm.shape[2]
    me = lax.axis_index("x").astype(jnp.int32)[None]
    depth = n_z * rows
    return kernel_call(
        functools.partial(by_x_kernel, n_x, n_z),
        [((n_y * n_c, rows, depth), grm.dtype)] * n_x,
        [me, grm.reshape(n_y * n_c, rows, n_x * depth)],
        1,
    )


def rearranged(blocks, ready):
    n_y, n_c, _, n_x = (lax.axis_size(name) for name in HI_LO)
    _, rows, depth = blocks[0].shape
    me = jnp.stack([lax.axis_index("x"), lax.axis_index("c")]).astype(jnp.int32)
    arrived = [shifted(block, "x", k) if k else block for k, block in enumerate(blocks)]
    kept, other = kernel_call(
        functools.partial(place_kernel, n_x, n_c),
        [((n_y, n_x, rows, depth), BF16)] * 2,
        [me, *arrived],
        1,
    )
    other, *ready = lax.optimization_barrier((other, *ready))
    return (kept.reshape(-1, depth), shifted(other, "c", 1).reshape(-1, depth)), ready


def times_kernel(rows, width, share, rank, me_ref, g_near_ref, g_far_ref, near_ref, far_ref, *refs):
    near_field_ref, far_field_ref, below_ref = refs[-3:]
    out_ref, own_ref = refs[-5:-3]
    step = pl.program_id(0)

    @pl.when(step == 0)
    def _():
        for half, field_ref in ((near_ref, near_field_ref), (far_ref, far_field_ref)):
            for z in range(half.shape[0]):
                field_ref[z * rows : (z + 1) * rows] = half[z, :rows, :width]

    product = jnp.dot(g_near_ref[...], near_field_ref[...], preferred_element_type=F32)
    product += jnp.dot(g_far_ref[...], far_field_ref[...], preferred_element_type=F32)
    per_step = out_ref.shape[0]
    for k in range(per_step):
        block = product[k * rows : (k + 1) * rows]
        out_ref[k, :rows] = block.astype(BF16)

        @pl.when(me_ref[0] == step * per_step + k)
        def _():
            own_ref[...] = block

    if share:

        @pl.when(step == 0)
        def _():
            t_ref, near_k_ref, far_k_ref, near_first_ref, far_first_ref = refs[:5]
            depth = near_ref.shape[0] * rows
            images = [
                half[:, :rows, half.shape[2] - rank :].reshape(depth, rank)
                for half in (near_k_ref, far_k_ref)
            ]
            firsts = [
                half[:, :rows, :width].reshape(depth, width)
                for half in (near_first_ref, far_first_ref)
            ]
            values = [t_ref[...]]
            for others in (firsts, (near_field_ref[...], far_field_ref[...])):
                total = sum(
                    lax.dot_general(
                        image, other, (((0,), (0,)), ((), ())), preferred_element_type=F32
                    )
                    for image, other in zip(images, others)
                )
                mine = jnp.zeros((share, width), F32)
                for i in range(rank // share):
                    mine = jnp.where(me_ref[1] == i, total[i * share : (i + 1) * share], mine)
                values.append(mine)
            below_ref[...] = jnp.concatenate(in_two(jnp.concatenate(values, axis=0)), axis=0)

        for k in range(per_step):
            out_ref[k, rows:] = below_ref[...]
    elif out_ref.shape[1] > rows:
        for k in range(per_step):
            out_ref[k, rows:] = refs[0][k]


def in_two(values):
    top = values.astype(BF16)
    return top, (values - top.astype(F32)).astype(BF16)


def send_coefficients(field, basis_ref, sent_refs):
    top, rest = in_two(field)
    terms = jnp.concatenate([top, rest, top], axis=0)
    coefficients = jnp.dot(basis_ref[...], terms, preferred_element_type=F32).astype(BF16)
    rank = sent_refs[0].shape[0]
    for bit, ref in enumerate(sent_refs):
        ref[...] = coefficients[bit * rank : (bit + 1) * rank]


def coefficients_kernel(field_ref, basis_ref, *sent_refs):
    send_coefficients(field_ref[...], basis_ref, sent_refs)


def image_kernel(with_coarse, me_ref, variance_ref, arrived_ref, own_ref, field_ref, *refs):
    rows = own_ref.shape[0]

    def add(d, total):
        part = arrived_ref[d, :rows].astype(F32)
        return total + jnp.where(me_ref[0] == d, jnp.zeros_like(part), part)

    total = lax.fori_loop(0, arrived_ref.shape[0], add, own_ref[...])
    image = variance_ref[0] * total + variance_ref[1] * field_ref[...]
    if len(refs) == 1:
        refs[0][...] = image
        return
    if not with_coarse:
        refs[1][...] = image
        send_coefficients(image, refs[0], refs[2:])
        return
    basis_ref, coupling_ref, image_ref, coarse_ref, s0_ref = refs[:5]
    rank = coupling_ref.shape[0]
    rhs = image.shape[1] - rank
    share = (arrived_ref.shape[1] - rows) // 6
    pieces = []
    for d in range(arrived_ref.shape[0]):
        rode = arrived_ref[d, rows:, :rhs].astype(F32)
        pieces.append(rode[:share] + rode[3 * share : 4 * share])
    t0 = jnp.concatenate(pieces, axis=0)
    s0 = jnp.dot(coupling_ref[...], t0, precision=EXACT, preferred_element_type=F32)
    coarse = image[:, rhs:]
    image = image[:, :rhs] + jnp.dot(coarse, s0, precision=EXACT, preferred_element_type=F32)
    image_ref[...] = image
    coarse_ref[...] = coarse
    s0_ref[...] = s0
    send_coefficients(image, basis_ref, refs[5:])


def lift_kernel(levels, cuts, inside, field_ref, own_ref, lift_ref, *refs):
    outs = refs[-2 * len(cuts) :]
    arrived, extra = refs[:levels], refs[levels : -2 * len(cuts)]
    rank = arrived[0].shape[0]
    rows = field_ref.shape[0]
    terms = sum(
        jnp.dot(
            lift_ref[:, bit * rank : (bit + 1) * rank],
            arrived[bit][...],
            preferred_element_type=F32,
        )
        for bit in range(levels)
    )
    field = jnp.dot(own_ref[...], field_ref[...], precision=EXACT, preferred_element_type=F32)
    field = field + (terms[:rows] + terms[rows:])
    beside = [ref for ref in extra if ref.shape[0] == rows]
    below = [ref for ref in extra if ref.shape[0] != rows]
    for k, (start, stop) in enumerate(cuts):
        out_ref, sent_ref = outs[2 * k : 2 * k + 2]
        part = field[:, start:stop]
        whole = part
        if beside and k == 0:
            whole = jnp.concatenate([part, beside[0][...]], axis=1)
        out_ref[...] = whole if inside else part
        whole = whole.astype(BF16)
        for copy in range(sent_ref.shape[0]):
            sent_ref[copy, :rows] = whole
            for ref in below:
                sent_ref[copy, rows:] = ref[...]


def kernel_call(kernel, shapes, operands, scalars=0, scratch=()):
    in_smem = [pl.BlockSpec(memory_space=pltpu.SMEM)] * scalars
    in_vmem = [pl.BlockSpec(memory_space=pltpu.VMEM)] * (len(operands) - scalars)
    return pl.pallas_call(
        kernel,
        out_shape=[jax.ShapeDtypeStruct(shape, dtype) for shape, dtype in shapes],
        in_specs=in_smem + in_vmem,
        out_specs=[pl.BlockSpec(memory_space=pltpu.VMEM)] * len(shapes),
        scratch_shapes=[pltpu.VMEM(shape, dtype) for shape, dtype in scratch],
        interpret=INTERPRET,
    )(*operands)


def local(grm, right_sides, inv_diag, bases, couplings, level_map, variance, iters_per_column):
    rows, rhs = right_sides.shape
    levels = couplings.shape[0] - 1
    rank = couplings.shape[1]
    split_at = levels * rank
    width = rhs + rank
    n_rows, n_columns = lax.axis_size(ROWS), lax.axis_size(COLUMNS)
    me_rows, me_columns = lax.axis_index(ROWS), lax.axis_index(COLUMNS)

    old = lax.broadcasted_iota(jnp.int32, (split_at, split_at), 0)
    new = jnp.repeat(level_map, rank) * rank + jnp.arange(split_at, dtype=jnp.int32) % rank
    shuffle = (old == new[None, :]).astype(F32)
    by_bit = mm3(bases[:, :split_at], shuffle)
    coarse_basis = bases[:, split_at:]

    scale = 1.0 / (n_rows * n_columns * jnp.max(jnp.abs(couplings)))
    couplings = couplings * scale
    diag = (inv_diag * scale)[:, None]
    coarse_coupling = couplings[levels]
    column = lax.broadcasted_iota(jnp.int32, (split_at, split_at), 1)
    repeat = (
        lax.broadcasted_iota(jnp.int32, (rank, split_at), 0)
        == lax.broadcasted_iota(jnp.int32, (rank, split_at), 1) % rank
    )
    tiled = mm3(couplings[:levels].reshape(split_at, rank), repeat.astype(F32))
    old_rows = lax.broadcasted_iota(jnp.int32, (split_at, split_at), 0)
    diagonal_blocks = jnp.where(old_rows // rank == column // rank, tiled, 0.0)
    lift = mm3(mm3(bases[:, :split_at], diagonal_blocks), shuffle)
    lift_terms = two_terms(lift)
    eye = lax.broadcasted_iota(jnp.int32, (rows, rows), 0) == jnp.arange(rows)[None]
    own_lift = mm3(lift, by_bit.T) + jnp.where(eye, diag, 0.0)
    basis_top, basis_rest = jnp.split(two_terms(by_bit.T), 2, axis=0)
    basis_terms = jnp.concatenate([basis_top, basis_top, basis_rest], axis=1)

    def coefficient_shapes(columns):
        return [((rank, columns), BF16)] * levels

    def precondition(field, sent, cuts=None, inside=False, beside=None, below=None):
        far = [("x", 1), ("x", 2), ("z", 1), ("z", 2), ("z", 4), ("c", 1), ("y", 1), ("y", 2)]
        order = [4, 3, 7, 1, 2, 6, 0, 5]
        arrived = {bit: from_partner(sent[bit], *far[bit]) for bit in order}
        extra = [array for array in (beside, below) if array is not None]
        more_rows = 0 if below is None else below.shape[0]
        cuts = cuts or [(0, field.shape[1])]
        shapes = []
        for k, (start, stop) in enumerate(cuts):
            more = beside.shape[1] if beside is not None and k == 0 else 0
            shapes.append(((rows, stop - start + (more if inside else 0)), F32))
            copies = (lax.axis_size("z"), rows + more_rows, stop - start + more)
            shapes.append((copies, BF16))
        return kernel_call(
            functools.partial(lift_kernel, levels, cuts, inside),
            shapes,
            [field, own_lift, lift_terms, *[arrived[bit] for bit in range(levels)], *extra],
        )

    places = jnp.stack([me_rows, me_columns]).astype(jnp.int32)
    right_sides, *blocks = lax.optimization_barrier((right_sides, *cut_by_x(grm)))
    sent = kernel_call(coefficients_kernel, coefficient_shapes(rhs), [right_sides, basis_terms])
    share = rank // n_columns
    t_share = rank // n_rows
    t_parts = mm3(coarse_basis.T, right_sides).reshape(n_rows, t_share, rhs)
    t_top = lax.reduce_precision(t_parts, 8, 7)
    t_parts = jnp.concatenate([t_top, t_parts - t_top], axis=1).astype(BF16)
    t_parts = jnp.pad(t_parts, ((0, 0), (0, 0), (0, rank)))
    g_blocks, (t_parts, places) = rearranged(blocks, (t_parts, places))

    def gathered(copies):
        near = exchanged(copies, "z")
        return near, shifted(near, "c", 1)

    def products(everyone, width, riders=(), more_rows=0, share=0):
        depth = lax.axis_size("z") * rows
        per_step = n_rows // 2
        height = rows + more_rows

        def whole(array):
            return pl.BlockSpec(array.shape, lambda i: (0,) * array.ndim)

        def some(shape):
            return pl.BlockSpec(shape, lambda i: (i,) + (0,) * (len(shape) - 1))

        rider_specs = [whole(array) for array in riders]
        if riders and not share:
            rider_specs = [some((per_step, *riders[0].shape[1:]))]
        partial, own = pl.pallas_call(
            functools.partial(times_kernel, rows, width, share, rank),
            grid=(2,),
            out_shape=[
                jax.ShapeDtypeStruct((n_rows, height, width), BF16),
                jax.ShapeDtypeStruct((rows, width), F32),
            ],
            in_specs=[
                pl.BlockSpec(memory_space=pltpu.SMEM),
                *[some((per_step * rows, depth))] * 2,
                *[whole(array) for array in everyone],
                *rider_specs,
            ],
            out_specs=[some((per_step, height, width)), pl.BlockSpec((rows, width), lambda i: (0, 0))],
            scratch_shapes=[
                *[pltpu.VMEM((depth, width), BF16)] * 2,
                pltpu.VMEM((more_rows or 8, width), BF16),
            ],
            name="times",
            interpret=INTERPRET,
        )(places, *g_blocks, *everyone, *riders)
        return exchanged(partial, ROWS), own

    def image_of(arrived, own, field):
        width = field.shape[1]
        operands = [places, variance, arrived, own, field, basis_terms]
        shapes = [((rows, width), F32)] + coefficient_shapes(width)
        kernel = functools.partial(image_kernel, False)
        image, *sent = kernel_call(kernel, shapes, operands, 2)
        return image, sent

    def last_image_of(arrived, own, field):
        operands = [places, variance, arrived, own, field]
        kernel = functools.partial(image_kernel, False)
        return kernel_call(kernel, [(field.shape, F32)], operands, 2)[0]

    def image_with_coarse(arrived, own, field):
        operands = [places, variance, arrived, own, field, basis_terms, coarse_coupling]
        shapes = [((rows, rhs), F32), ((rows, rank), F32), ((rank, rhs), F32)]
        kernel = functools.partial(image_kernel, True)
        shapes = shapes + coefficient_shapes(rhs)
        image, coarse, s0, *sent = kernel_call(kernel, shapes, operands, 2)
        return image, coarse, s0, sent

    def sum_of_terms(terms, axis):
        top, rest = jnp.split(terms.astype(F32), 2, axis=axis)
        return top + rest

    def padded(array, width):
        more = width - array.shape[-1]
        return jnp.pad(array, [(0, 0)] * (array.ndim - 1) + [(0, more)])

    cuts = [(0, rhs)]
    first, copies = precondition(right_sides, sent, cuts, True, beside=coarse_basis)
    all_first = gathered(copies)
    arrived, own = products(all_first, width, [t_parts], 2 * t_share)
    first_image, sent = image_of(arrived, own, first)
    coarse_image = first_image[:, rhs:]

    t_rows = sum_of_terms(arrived[:, rows:], 1).sum(axis=0)
    t_rows = two_terms(padded(t_rows, width + rank))
    second, copies = precondition(first_image, sent, beside=coarse_image, below=t_rows)
    all_second = gathered(copies)
    near, far = all_second
    t_rows = near[:, rows:, :width].astype(F32) + far[:, rows:, :width].astype(F32)
    t_rows = sum_of_terms(t_rows, 1).sum(axis=0)
    riders = [t_rows, *all_second, *all_first]
    arrived, own = products(all_second, width, riders, 6 * share, share)
    second_image, second_coarse, s0, sent = image_with_coarse(arrived, own, second)

    rode = sum_of_terms(arrived[:, rows:], 1)[:, t_share:].sum(axis=0)
    below = [rode[:, :rhs], rode[:, rhs:].reshape(-1, rhs)]
    below = two_terms(jnp.concatenate(below, axis=0))
    n_below = below.shape[0]
    below = jnp.pad(below, ((0, -n_below % 8), (0, 0)))
    third, copies = precondition(second_image, sent, below=below)
    everyone = gathered(copies)
    arrived, own = products(everyone, rhs)
    own, *everyone = lax.optimization_barrier((own, *everyone))
    third_image = last_image_of(arrived, own, third)

    table = sum_of_terms(jnp.stack([array[:, rows : rows + n_below] for array in everyone]), 2)
    table = jnp.where(lax.axis_index("c") == 0, table, table[::-1])
    table = table.reshape(n_columns, n_below // 2, rhs)
    k_first = table[:, :share].reshape(rank, rhs)
    k_second = table[:, share : 2 * share].reshape(rank, rhs)
    k_coarse = table[:, 2 * share :].reshape(n_columns, 2, share, rank).transpose(1, 0, 2, 3)
    k_basis, k_coarse = k_coarse.reshape(2, rank, rank)
    s1 = mm(coarse_coupling, k_first + mm(k_basis, s0))
    s2 = mm(coarse_coupling, k_second + mm(k_coarse, s0) + mm(k_basis, s1))
    weights = jnp.concatenate([s0, s1, s2], axis=0)

    none = jnp.zeros_like(coarse_basis)
    second_lift = second[:, rhs:]
    coarse_parts = [
        [coarse_basis, none, none],
        [second_lift, coarse_basis, none],
        [none, second_lift, coarse_basis],
        [coarse_image, none, none],
        [none, coarse_image, none],
        [none, second_coarse, coarse_image],
    ]
    coarse_parts = jnp.concatenate([jnp.concatenate(row, axis=1) for row in coarse_parts], axis=0)
    coarse_parts = mm3(coarse_parts, weights).reshape(6, rows, rhs)
    fields = [first[:, :rhs], second[:, :rhs], third]
    v = [field + part for field, part in zip(fields, coarse_parts[:3])]
    fields = [first_image[:, :rhs], second_image, third_image]
    w = [right_sides] + [field + part for field, part in zip(fields, coarse_parts[3:])]

    moments = jnp.stack([jnp.sum(w[k - k // 2] * v[k // 2], axis=0) for k in range(2 * STEPS)])
    moments = from_everyone(moments, ROWS).sum(axis=0)
    moments = from_everyone(moments, COLUMNS).sum(axis=0)

    m = [moments[k] for k in range(2 * STEPS)]
    one, zero = jnp.ones_like(m[0]), jnp.zeros_like(m[0])
    in_r, kept_r, kept_x, direction, energy = [one], [one], [], [], None
    for step in range(STEPS):
        basis = range(step + 1)
        fresh = sum(in_r[p] * in_r[q] * m[p + q] for p in basis for q in basis)
        before = [fresh / energy * d for d in direction] if step else []
        direction = [r + d for r, d in zip(in_r, before + [zero])]
        energy = fresh
        alpha = energy / sum(direction[p] * direction[q] * m[p + q + 1] for p in basis for q in basis)
        in_r = [a - b for a, b in zip(in_r + [zero], [zero] + [alpha * d for d in direction])]
        active = step < iters_per_column
        kept_r = [jnp.where(active, a, b) for a, b in zip(in_r, kept_r + [zero])]
        kept_x = [jnp.where(active, b + alpha * d, b) for d, b in zip(direction, kept_x + [zero])]

    solution = sum(c * field for c, field in zip(kept_x, v))
    residual = w[0] + sum(c * field for c, field in zip(kept_r[1:], w[1:]))
    return (solution, residual)


def solution(mesh):
    split = Mesh(mesh.devices.reshape(4, 2, 8, 4), HI_LO)
    return jax.shard_map(
        local,
        mesh=split,
        in_specs=(
            P(None, LO, None, HI, None),
            P(HI_LO, None),
            P(HI_LO),
            P(HI_LO, None),
            P(),
            P(),
            P(),
            P(),
        ),
        out_specs=(P(HI_LO, None), P(HI_LO, None)),
        check_vma=False,
    )
```

```python
import functools

import jax
import jax.numpy as jnp
from jax import lax
from jax.experimental import pallas as pl
from jax.experimental.pallas import tpu as pltpu
from jax.sharding import Mesh
from jax.sharding import PartitionSpec as P


HI = ("y", "c")
LO = ("z", "x")
HI_LO = ("y", "c", "z", "x")
COLUMNS = ("c", "z")
ROWS = ("y", "x")
BF16 = jnp.bfloat16
F32 = jnp.float32
EXACT = lax.Precision.HIGHEST
STEPS = 3
INTERPRET = False


def mm(left, right):
    return jnp.dot(left, right, precision=EXACT)


def mm3(left, right):
    return jnp.dot(left, right, precision=lax.Precision.HIGH)


def from_everyone(array, axes):
    copies = jnp.broadcast_to(array, (lax.axis_size(axes), *array.shape))
    return lax.all_to_all(copies, axes, split_axis=0, concat_axis=0, tiled=True)


def exchanged(array, axes):
    return lax.all_to_all(array, axes, split_axis=0, concat_axis=0, tiled=True)


def shifted(value, axis, step):
    size = lax.axis_size(axis)
    return lax.ppermute(value, axis, [(i, (i + step) % size) for i in range(size)])


def from_partner(value, axis, distance):
    return lax.ppermute(value, axis, [(i, i ^ distance) for i in range(lax.axis_size(axis))])


def two_terms(values):
    top = lax.reduce_precision(values, 8, 7)
    return jnp.concatenate([top, values - top], axis=0).astype(BF16)


def by_x_kernel(n_x, n_z, me_ref, grm_ref, *out_refs):
    rows = grm_ref.shape[1]

    def regroup(block, _):
        whole = grm_ref[block]
        columns = []
        for x in range(n_x):
            starts = [(z * n_x + x) * rows for z in range(n_z)]
            columns.append(jnp.concatenate([whole[:, at : at + rows] for at in starts], axis=1))
        for step, out_ref in enumerate(out_refs):
            wanted = lax.rem(me_ref[0] + step, n_x)
            chosen = columns[0]
            for x in range(1, n_x):
                chosen = jnp.where(wanted == x, columns[x], chosen)
            out_ref[block] = chosen
        return 0

    lax.fori_loop(0, grm_ref.shape[0], regroup, 0)


def place_kernel(n_x, n_c, me_ref, *refs):
    arrived, (kept_ref, other_ref) = refs[:n_x], refs[n_x:]
    for step, ref in enumerate(arrived):
        x = lax.rem(me_ref[0] - step + n_x, n_x)
        for y in range(ref.shape[0] // n_c):
            kept_ref[y, x] = ref[y * n_c + me_ref[1]]
            other_ref[y, x] = ref[y * n_c + 1 - me_ref[1]]


def cut_by_x(grm):
    n_y, n_c, n_z, n_x = (lax.axis_size(name) for name in HI_LO)
    rows = grm.shape[2]
    me = lax.axis_index("x").astype(jnp.int32)[None]
    depth = n_z * rows
    return kernel_call(
        functools.partial(by_x_kernel, n_x, n_z),
        [((n_y * n_c, rows, depth), grm.dtype)] * n_x,
        [me, grm.reshape(n_y * n_c, rows, n_x * depth)],
        1,
    )


def rearranged(blocks, ready):
    n_y, n_c, _, n_x = (lax.axis_size(name) for name in HI_LO)
    _, rows, depth = blocks[0].shape
    me = jnp.stack([lax.axis_index("x"), lax.axis_index("c")]).astype(jnp.int32)
    arrived = [shifted(block, "x", k) if k else block for k, block in enumerate(blocks)]
    kept, other = kernel_call(
        functools.partial(place_kernel, n_x, n_c),
        [((n_y, n_x, rows, depth), BF16)] * 2,
        [me, *arrived],
        1,
    )
    other, *ready = lax.optimization_barrier((other, *ready))
    return (kept.reshape(-1, depth), shifted(other, "c", 1).reshape(-1, depth)), ready


def times_kernel(rows, width, share, rank, me_ref, g_near_ref, g_far_ref, near_ref, far_ref, *refs):
    near_field_ref, far_field_ref, below_ref = refs[-3:]
    out_ref, own_ref = refs[-5:-3]
    step = pl.program_id(0)

    @pl.when(step == 0)
    def _():
        for half, field_ref in ((near_ref, near_field_ref), (far_ref, far_field_ref)):
            for z in range(half.shape[0]):
                field_ref[z * rows : (z + 1) * rows] = half[z, :rows, :width]

    product = jnp.dot(g_near_ref[...], near_field_ref[...], preferred_element_type=F32)
    product += jnp.dot(g_far_ref[...], far_field_ref[...], preferred_element_type=F32)
    per_step = out_ref.shape[0]
    for k in range(per_step):
        block = product[k * rows : (k + 1) * rows]
        sent = block.astype(BF16)
        if out_ref.shape[2] > width:
            sent = jnp.concatenate([sent, refs[0][k]], axis=1)
        out_ref[k, :rows] = sent

        @pl.when(me_ref[0] == step * per_step + k)
        def _():
            own_ref[...] = block

    if share:

        @pl.when(step == 0)
        def _():
            t_ref, near_k_ref, far_k_ref, near_first_ref, far_first_ref = refs[:5]
            depth = near_ref.shape[0] * rows
            images = [
                half[:, :rows, half.shape[2] - rank :].reshape(depth, rank)
                for half in (near_k_ref, far_k_ref)
            ]
            firsts = [
                half[:, :rows, :width].reshape(depth, width)
                for half in (near_first_ref, far_first_ref)
            ]
            values = [t_ref[...]]
            for others in (firsts, (near_field_ref[...], far_field_ref[...])):
                total = sum(
                    lax.dot_general(
                        image, other, (((0,), (0,)), ((), ())), preferred_element_type=F32
                    )
                    for image, other in zip(images, others)
                )
                mine = jnp.zeros((share, width), F32)
                for i in range(rank // share):
                    mine = jnp.where(me_ref[1] == i, total[i * share : (i + 1) * share], mine)
                values.append(mine)
            below_ref[...] = jnp.concatenate(in_two(jnp.concatenate(values, axis=0)), axis=0)

        for k in range(per_step):
            out_ref[k, rows:] = below_ref[...]


def in_two(values):
    top = values.astype(BF16)
    return top, (values - top.astype(F32)).astype(BF16)


def send_coefficients(field, basis_ref, sent_refs):
    top, rest = in_two(field)
    terms = jnp.concatenate([top, rest, top], axis=0)
    coefficients = jnp.dot(basis_ref[...], terms, preferred_element_type=F32).astype(BF16)
    rank = sent_refs[0].shape[0]
    for bit, ref in enumerate(sent_refs):
        ref[...] = coefficients[bit * rank : (bit + 1) * rank]


def coefficients_kernel(field_ref, basis_ref, *sent_refs):
    send_coefficients(field_ref[...], basis_ref, sent_refs)


def image_kernel(with_coarse, me_ref, variance_ref, arrived_ref, own_ref, field_ref, *refs):
    rows = own_ref.shape[0]

    def add(d, total):
        part = arrived_ref[d, :rows, : own_ref.shape[1]].astype(F32)
        return total + jnp.where(me_ref[0] == d, jnp.zeros_like(part), part)

    total = lax.fori_loop(0, arrived_ref.shape[0], add, own_ref[...])
    image = variance_ref[0] * total + variance_ref[1] * field_ref[...]
    if len(refs) == 1:
        refs[0][...] = image
        return
    if not with_coarse:
        refs[1][...] = image
        send_coefficients(image, refs[0], refs[2:])
        return
    basis_ref, coupling_ref, image_ref, coarse_ref, s0_ref = refs[:5]
    rank = coupling_ref.shape[0]
    rhs = image.shape[1] - rank
    share = (arrived_ref.shape[1] - rows) // 6
    pieces = []
    for d in range(arrived_ref.shape[0]):
        rode = arrived_ref[d, rows:, :rhs].astype(F32)
        pieces.append(rode[:share] + rode[3 * share : 4 * share])
    t0 = jnp.concatenate(pieces, axis=0)
    s0 = jnp.dot(coupling_ref[...], t0, precision=EXACT, preferred_element_type=F32)
    coarse = image[:, rhs:]
    image = image[:, :rhs] + jnp.dot(coarse, s0, precision=EXACT, preferred_element_type=F32)
    image_ref[...] = image
    coarse_ref[...] = coarse
    s0_ref[...] = s0
    send_coefficients(image, basis_ref, refs[5:])


def lift_kernel(levels, cuts, inside, field_ref, own_ref, lift_ref, *refs):
    outs = refs[-2 * len(cuts) :]
    arrived, extra = refs[:levels], refs[levels : -2 * len(cuts)]
    rank = arrived[0].shape[0]
    rows = field_ref.shape[0]
    terms = sum(
        jnp.dot(
            lift_ref[:, bit * rank : (bit + 1) * rank],
            arrived[bit][...],
            preferred_element_type=F32,
        )
        for bit in range(levels)
    )
    field = jnp.dot(own_ref[...], field_ref[...], precision=EXACT, preferred_element_type=F32)
    field = field + (terms[:rows] + terms[rows:])
    beside = [ref for ref in extra if ref.shape[0] == rows]
    below = [ref for ref in extra if ref.shape[0] != rows]
    for k, (start, stop) in enumerate(cuts):
        out_ref, sent_ref = outs[2 * k : 2 * k + 2]
        part = field[:, start:stop]
        whole = part
        if beside and k == 0:
            whole = jnp.concatenate([part, beside[0][...]], axis=1)
        out_ref[...] = whole if inside else part
        whole = whole.astype(BF16)
        for copy in range(sent_ref.shape[0]):
            sent_ref[copy, :rows] = whole
            for ref in below:
                sent_ref[copy, rows:] = ref[...]


def kernel_call(kernel, shapes, operands, scalars=0, scratch=()):
    in_smem = [pl.BlockSpec(memory_space=pltpu.SMEM)] * scalars
    in_vmem = [pl.BlockSpec(memory_space=pltpu.VMEM)] * (len(operands) - scalars)
    return pl.pallas_call(
        kernel,
        out_shape=[jax.ShapeDtypeStruct(shape, dtype) for shape, dtype in shapes],
        in_specs=in_smem + in_vmem,
        out_specs=[pl.BlockSpec(memory_space=pltpu.VMEM)] * len(shapes),
        scratch_shapes=[pltpu.VMEM(shape, dtype) for shape, dtype in scratch],
        interpret=INTERPRET,
    )(*operands)


def local(grm, right_sides, inv_diag, bases, couplings, level_map, variance, iters_per_column):
    rows, rhs = right_sides.shape
    levels = couplings.shape[0] - 1
    rank = couplings.shape[1]
    split_at = levels * rank
    width = rhs + rank
    n_rows, n_columns = lax.axis_size(ROWS), lax.axis_size(COLUMNS)
    me_rows, me_columns = lax.axis_index(ROWS), lax.axis_index(COLUMNS)

    old = lax.broadcasted_iota(jnp.int32, (split_at, split_at), 0)
    new = jnp.repeat(level_map, rank) * rank + jnp.arange(split_at, dtype=jnp.int32) % rank
    shuffle = (old == new[None, :]).astype(F32)
    by_bit = mm3(bases[:, :split_at], shuffle)
    coarse_basis = bases[:, split_at:]

    scale = 1.0 / (n_rows * n_columns * jnp.max(jnp.abs(couplings)))
    couplings = couplings * scale
    diag = (inv_diag * scale)[:, None]
    coarse_coupling = couplings[levels]
    column = lax.broadcasted_iota(jnp.int32, (split_at, split_at), 1)
    repeat = (
        lax.broadcasted_iota(jnp.int32, (rank, split_at), 0)
        == lax.broadcasted_iota(jnp.int32, (rank, split_at), 1) % rank
    )
    tiled = mm3(couplings[:levels].reshape(split_at, rank), repeat.astype(F32))
    old_rows = lax.broadcasted_iota(jnp.int32, (split_at, split_at), 0)
    diagonal_blocks = jnp.where(old_rows // rank == column // rank, tiled, 0.0)
    lift = mm3(mm3(bases[:, :split_at], diagonal_blocks), shuffle)
    lift_terms = two_terms(lift)
    eye = lax.broadcasted_iota(jnp.int32, (rows, rows), 0) == jnp.arange(rows)[None]
    own_lift = mm3(lift, by_bit.T) + jnp.where(eye, diag, 0.0)
    basis_top, basis_rest = jnp.split(two_terms(by_bit.T), 2, axis=0)
    basis_terms = jnp.concatenate([basis_top, basis_top, basis_rest], axis=1)

    def coefficient_shapes(columns):
        return [((rank, columns), BF16)] * levels

    def precondition(field, sent, cuts=None, inside=False, beside=None, below=None):
        far = [("x", 1), ("x", 2), ("z", 1), ("z", 2), ("z", 4), ("c", 1), ("y", 1), ("y", 2)]
        order = [4, 3, 7, 1, 2, 6, 0, 5]
        arrived = {bit: from_partner(sent[bit], *far[bit]) for bit in order}
        extra = [array for array in (beside, below) if array is not None]
        more_rows = 0 if below is None else below.shape[0]
        cuts = cuts or [(0, field.shape[1])]
        shapes = []
        for k, (start, stop) in enumerate(cuts):
            more = beside.shape[1] if beside is not None and k == 0 else 0
            shapes.append(((rows, stop - start + (more if inside else 0)), F32))
            copies = (lax.axis_size("z"), rows + more_rows, stop - start + more)
            shapes.append((copies, BF16))
        return kernel_call(
            functools.partial(lift_kernel, levels, cuts, inside),
            shapes,
            [field, own_lift, lift_terms, *[arrived[bit] for bit in range(levels)], *extra],
        )

    places = jnp.stack([me_rows, me_columns]).astype(jnp.int32)
    right_sides, *blocks = lax.optimization_barrier((right_sides, *cut_by_x(grm)))
    sent = kernel_call(coefficients_kernel, coefficient_shapes(rhs), [right_sides, basis_terms])
    share = rank // n_columns
    t_share = rank // n_rows
    t_parts = mm3(coarse_basis.T, right_sides).reshape(n_rows, t_share, rhs)
    t_top = lax.reduce_precision(t_parts, 8, 7)
    t_parts = jnp.concatenate([t_top, t_parts - t_top], axis=1).astype(BF16)
    t_parts = t_parts.reshape(n_rows, -1, rank)
    t_height = t_parts.shape[1]
    t_parts = jnp.pad(t_parts, ((0, 0), (0, rows - t_height), (0, 0)))
    g_blocks, (t_parts, places) = rearranged(blocks, (t_parts, places))

    def gathered(copies):
        near = exchanged(copies, "z")
        return near, shifted(near, "c", 1)

    def products(everyone, width, riders=(), more_rows=0, share=0, more_columns=0):
        depth = lax.axis_size("z") * rows
        per_step = n_rows // 2
        height = rows + more_rows

        def whole(array):
            return pl.BlockSpec(array.shape, lambda i: (0,) * array.ndim)

        def some(shape):
            return pl.BlockSpec(shape, lambda i: (i,) + (0,) * (len(shape) - 1))

        rider_specs = [whole(array) for array in riders]
        if riders and not share:
            rider_specs = [some((per_step, *riders[0].shape[1:]))]
        partial, own = pl.pallas_call(
            functools.partial(times_kernel, rows, width, share, rank),
            grid=(2,),
            out_shape=[
                jax.ShapeDtypeStruct((n_rows, height, width + more_columns), BF16),
                jax.ShapeDtypeStruct((rows, width), F32),
            ],
            in_specs=[
                pl.BlockSpec(memory_space=pltpu.SMEM),
                *[some((per_step * rows, depth))] * 2,
                *[whole(array) for array in everyone],
                *rider_specs,
            ],
            out_specs=[some((per_step, height, width + more_columns)), pl.BlockSpec((rows, width), lambda i: (0, 0))],
            scratch_shapes=[
                *[pltpu.VMEM((depth, width), BF16)] * 2,
                pltpu.VMEM((more_rows or 8, width), BF16),
            ],
            name="times",
            interpret=INTERPRET,
        )(places, *g_blocks, *everyone, *riders)
        return exchanged(partial, ROWS), own

    def image_of(arrived, own, field):
        width = field.shape[1]
        operands = [places, variance, arrived, own, field, basis_terms]
        shapes = [((rows, width), F32)] + coefficient_shapes(width)
        kernel = functools.partial(image_kernel, False)
        image, *sent = kernel_call(kernel, shapes, operands, 2)
        return image, sent

    def last_image_of(arrived, own, field):
        operands = [places, variance, arrived, own, field]
        kernel = functools.partial(image_kernel, False)
        return kernel_call(kernel, [(field.shape, F32)], operands, 2)[0]

    def image_with_coarse(arrived, own, field):
        operands = [places, variance, arrived, own, field, basis_terms, coarse_coupling]
        shapes = [((rows, rhs), F32), ((rows, rank), F32), ((rank, rhs), F32)]
        kernel = functools.partial(image_kernel, True)
        shapes = shapes + coefficient_shapes(rhs)
        image, coarse, s0, *sent = kernel_call(kernel, shapes, operands, 2)
        return image, coarse, s0, sent

    def sum_of_terms(terms, axis):
        top, rest = jnp.split(terms.astype(F32), 2, axis=axis)
        return top + rest

    def padded(array, width):
        more = width - array.shape[-1]
        return jnp.pad(array, [(0, 0)] * (array.ndim - 1) + [(0, more)])

    cuts = [(0, rhs)]
    first, copies = precondition(right_sides, sent, cuts, True, beside=coarse_basis)
    all_first = gathered(copies)
    arrived, own = products(all_first, width, [t_parts], more_columns=rank)
    first_image, sent = image_of(arrived, own, first)
    coarse_image = first_image[:, rhs:]

    t_rows = arrived[:, :t_height, width:].reshape(n_rows, 2 * t_share, rhs)
    t_rows = sum_of_terms(t_rows, 1).sum(axis=0)
    t_rows = two_terms(padded(t_rows, width + rank))
    second, copies = precondition(first_image, sent, beside=coarse_image, below=t_rows)
    all_second = gathered(copies)
    near, far = all_second
    t_rows = near[:, rows:, :width].astype(F32) + far[:, rows:, :width].astype(F32)
    t_rows = sum_of_terms(t_rows, 1).sum(axis=0)
    riders = [t_rows, *all_second, *all_first]
    arrived, own = products(all_second, width, riders, 6 * share, share)
    second_image, second_coarse, s0, sent = image_with_coarse(arrived, own, second)

    rode = sum_of_terms(arrived[:, rows:], 1)[:, t_share:].sum(axis=0)
    below = [rode[:, :rhs], rode[:, rhs:].reshape(-1, rhs)]
    below = two_terms(jnp.concatenate(below, axis=0))
    n_below = below.shape[0]
    below = jnp.pad(below, ((0, -n_below % 8), (0, 0)))
    third, copies = precondition(second_image, sent, below=below)
    everyone = gathered(copies)
    arrived, own = products(everyone, rhs)
    own, *everyone = lax.optimization_barrier((own, *everyone))
    third_image = last_image_of(arrived, own, third)

    table = sum_of_terms(jnp.stack([array[:, rows : rows + n_below] for array in everyone]), 2)
    table = jnp.where(lax.axis_index("c") == 0, table, table[::-1])
    table = table.reshape(n_columns, n_below // 2, rhs)
    k_first = table[:, :share].reshape(rank, rhs)
    k_second = table[:, share : 2 * share].reshape(rank, rhs)
    k_coarse = table[:, 2 * share :].reshape(n_columns, 2, share, rank).transpose(1, 0, 2, 3)
    k_basis, k_coarse = k_coarse.reshape(2, rank, rank)
    s1 = mm(coarse_coupling, k_first + mm(k_basis, s0))
    s2 = mm(coarse_coupling, k_second + mm(k_coarse, s0) + mm(k_basis, s1))
    weights = jnp.concatenate([s0, s1, s2], axis=0)

    none = jnp.zeros_like(coarse_basis)
    second_lift = second[:, rhs:]
    coarse_parts = [
        [coarse_basis, none, none],
        [second_lift, coarse_basis, none],
        [none, second_lift, coarse_basis],
        [coarse_image, none, none],
        [none, coarse_image, none],
        [none, second_coarse, coarse_image],
    ]
    coarse_parts = jnp.concatenate([jnp.concatenate(row, axis=1) for row in coarse_parts], axis=0)
    coarse_parts = mm3(coarse_parts, weights).reshape(6, rows, rhs)
    fields = [first[:, :rhs], second[:, :rhs], third]
    v = [field + part for field, part in zip(fields, coarse_parts[:3])]
    fields = [first_image[:, :rhs], second_image, third_image]
    w = [right_sides] + [field + part for field, part in zip(fields, coarse_parts[3:])]

    moments = jnp.stack([jnp.sum(w[k - k // 2] * v[k // 2], axis=0) for k in range(2 * STEPS)])
    moments = from_everyone(moments, ROWS).sum(axis=0)
    moments = from_everyone(moments, COLUMNS).sum(axis=0)

    m = [moments[k] for k in range(2 * STEPS)]
    one, zero = jnp.ones_like(m[0]), jnp.zeros_like(m[0])
    in_r, kept_r, kept_x, direction, energy = [one], [one], [], [], None
    for step in range(STEPS):
        basis = range(step + 1)
        fresh = sum(in_r[p] * in_r[q] * m[p + q] for p in basis for q in basis)
        before = [fresh / energy * d for d in direction] if step else []
        direction = [r + d for r, d in zip(in_r, before + [zero])]
        energy = fresh
        alpha = energy / sum(direction[p] * direction[q] * m[p + q + 1] for p in basis for q in basis)
        in_r = [a - b for a, b in zip(in_r + [zero], [zero] + [alpha * d for d in direction])]
        active = step < iters_per_column
        kept_r = [jnp.where(active, a, b) for a, b in zip(in_r, kept_r + [zero])]
        kept_x = [jnp.where(active, b + alpha * d, b) for d, b in zip(direction, kept_x + [zero])]

    solution = sum(c * field for c, field in zip(kept_x, v))
    residual = w[0] + sum(c * field for c, field in zip(kept_r[1:], w[1:]))
    return (solution, residual)


def solution(mesh):
    split = Mesh(mesh.devices.reshape(4, 2, 8, 4), HI_LO)
    return jax.shard_map(
        local,
        mesh=split,
        in_specs=(
            P(None, LO, None, HI, None),
            P(HI_LO, None),
            P(HI_LO),
            P(HI_LO, None),
            P(),
            P(),
            P(),
            P(),
        ),
        out_specs=(P(HI_LO, None), P(HI_LO, None)),
        check_vma=False,
    )
```
